128 devices in a mesh: blk: 32 (over z, y_hi, x), field: 4 (over y_lo, core).
Axes of the slice: x: 4, y: 4 (y_hi: 2, y_lo: 2; y = y_hi * 2 + y_lo), z: 4, core: 2. Of those that a mesh axis runs over, the one named last changes fastest.
Arguments:
- vectors: float32 [2048, 32768], P('blk', 'field'), may hold values from 0 to 10
- section: int32 [1], replicated, may hold values from 0 to 31
Outputs:
- metrics: float32 [2048, 4, 64], P('blk', None, 'field')
The draws below stay inside these ranges and needn't reach their ends.
All inputs are finite; a program needn't handle non-finite values.
Results may differ from the reference program's by a relative error of at most 0.0003.
Values sent between devices are 32-bit elements; how exact they have to be, the bound alone decides.
A program may use at most 64 MiB of HBM per device.

```python
import math
import jax
import jax.numpy as jnp
from jax import lax

FIELDS = 32768
V_DEV = 64
STEPS = 4
VECTORS = 2048
N_BLK = 32


def draw_vectors(key, part):
    folded = jax.random.fold_in(key, 17)
    key_rows, key_cols, key_cells, key_mix, key_pattern = jax.random.split(folded, 5)
    population = 8
    row_scale = jnp.exp(jax.random.uniform(key_rows, (VECTORS, 1), jnp.float32) * math.log(10.0))
    col_scale = jnp.exp(jax.random.uniform(key_cols, (1, FIELDS), jnp.float32) * math.log(10.0))
    patterns = jax.random.uniform(key_pattern, (population, FIELDS), jnp.float32)
    mixing = jax.random.uniform(key_mix, (VECTORS, population), jnp.float32) ** 4 + 0.01
    roughness = jax.random.uniform(key_cells, (VECTORS, FIELDS), jnp.float32, 0.25, 1.0)
    mixing = mixing / jnp.sum(mixing, axis=1, keepdims=True)
    blended = jnp.dot(mixing, patterns, precision=lax.Precision.HIGHEST)
    return (row_scale * col_scale * blended * roughness * 0.1).astype(jnp.float32)


def setup_inputs(seed: int = 0) -> dict:
    streams_of = jax.random.split(jax.random.key(seed), 3)
    return {
        "vectors": draw_vectors(jax.random.fold_in(streams_of[2], 71), 0),
        "section": jax.random.randint(streams_of[1], (1,), 0, N_BLK).astype(jnp.int32),
    }


def reference(vectors, section):
    sums = jnp.sum(vectors, axis=1)
    blocks = vectors.reshape(N_BLK, V_DEV, FIELDS)
    block_sums = sums.reshape(N_BLK, V_DEV)

    def one_block(index):
        own = blocks[index]
        own_sums = block_sums[index]

        def one_slot(slot):
            partner = (index + section[0] + slot) % N_BLK
            other = blocks[partner]
            other_sums = block_sums[partner]

            def one_row(row):
                return jnp.sum(jnp.minimum(row[None, :], other), axis=1)

            numer = lax.map(one_row, own)
            return 2.0 * numer / (own_sums[:, None] + other_sums[None, :])

        return lax.map(one_slot, jnp.arange(STEPS, dtype=jnp.int32))

    result = lax.map(one_block, jnp.arange(N_BLK, dtype=jnp.int32))
    return result.transpose(0, 2, 1, 3).reshape(N_BLK * V_DEV, STEPS, V_DEV)
```

```python
import jax
import jax.numpy as jnp
from jax import lax
from jax.experimental import pallas as pl
from jax.experimental.pallas import tpu as pltpu
from jax.sharding import Mesh
from jax.sharding import PartitionSpec as P

MESH = pl.DeviceIdType.MESH
AXES = ("z", "yh", "x", "yl", "core")
ROUNDS = 4
HALF = 128 // ROUNDS
NF = 2 * HALF
PITCH = NF + 8
TILES = 16
VREG = (8, 128)


def iota(axis):
    return lax.broadcasted_iota(jnp.int32, VREG, axis)


def spread(row):
    return jnp.broadcast_to(row, VREG)


def take(value, index):
    return jnp.take_along_axis(value, index, axis=1)


def kernel(
    section, x_hbm, out, xin, sent, got, rows, cols, roll_a, roll_b, acc, sums, core_in, plane_in, column_out, column_in,
    turn, load_sem, a_send, a_recv, c_send, c_recv, p_send, p_recv, y_send, y_recv,
):
    z, yh, x, yl, core = (lax.axis_index(name) for name in AXES)
    offset = section[0]
    block = z * 8 + yh * 4 + x
    column = yh * 2 + yl

    def blk_peer(e):
        return (lax.rem(z + e // 8, 4), lax.rem(yh + (e // 4) % 2, 2), lax.rem(x + e % 4, 4), yl, core)

    def plane_peer(e):
        return (lax.rem(z + e // 4, 4), yh, lax.rem(x + e % 4, 4), yl, core)

    def column_peer(d):
        y = lax.rem(column + d, 4)
        return (z, y // 2, x, lax.rem(y, 2), core)

    other_core = (z, yh, x, yl, 1 - core)

    loads = []
    for i in range(8):
        part = pl.ds(i * 1024, 1024)
        loads.append(pltpu.make_async_copy(x_hbm.at[:, part], xin.at[:, part], load_sem.at[i]))
        loads[-1].start()

    barrier = pltpu.get_barrier_semaphore()
    for e in range(1, 32):
        pl.semaphore_signal(barrier, inc=1, device_id=blk_peer(e), device_id_type=MESH)
    for peer in (column_peer(1), column_peer(3), other_core):
        pl.semaphore_signal(barrier, inc=1, device_id=peer, device_id_type=MESH)

    lane, sub = iota(1), iota(0)
    lane_c, lane_rho, lane_h = lane // 8, (lane // 2) % 4, lane % 2
    row_index = [lane_h * 64 + lane_rho * 16 + (lane_c + sub + 8 * q) % 16 for q in range(2)]
    col_index = [lane_h * 64 + g * 16 + lane_c for g in range(4)]

    for load in loads:
        load.wait()

    def transpose_one(u, _):
        left = xin[:, pl.ds(pl.multiple_of(u * 128, 128), 128)]
        right = xin[:, pl.ds(pl.multiple_of(u * 128 + 4096, 128), 128)]
        sent[u] = jnp.concatenate([left, right], axis=0).T
        return 0

    lax.fori_loop(0, 32, transpose_one, 0)
    got[block] = sent[block]
    for tile in range(32):
        sums[tile] = jnp.zeros(VREG, jnp.float32)

    def clear(tile, _):
        for c in range(2):
            for a in range(16):
                acc[tile, c, a] = jnp.zeros(VREG, jnp.float32)
        return 0

    lax.fori_loop(0, TILES, clear, 0)
    pl.semaphore_wait(barrier, 34)

    def a_copy(j, e):
        z2, yh2, x2, _, _ = blk_peer(e)
        part = pl.ds(pl.multiple_of(j * HALF, HALF), HALF)
        return pltpu.make_async_remote_copy(
            src_ref=sent.at[z2 * 8 + yh2 * 4 + x2, part],
            dst_ref=got.at[block, part],
            send_sem=a_send.at[j, e],
            recv_sem=a_recv.at[j, e],
            device_id=blk_peer(e),
            device_id_type=MESH,
        )

    def send_round(j, _):
        def send_one(i, _):
            a_copy(j, lax.rem(i * 13, 32)).start()
            return 0

        lax.fori_loop(1, 32, send_one, 0)
        return 0

    lax.fori_loop(0, ROUNDS, send_round, 0)

    def tile_at(i):
        e = lax.rem((15 - i) * 7, 16)
        return e, lax.rem(z + e // 4, 4) * 4 + lax.rem(x + e % 4, 4)

    def first_block(tile):
        return (tile // 4) * 8 + lax.rem(tile, 4)

    def arrange(j):
        def one(t, _):
            t4 = lax.rem(t + 4, 32)
            total = sums[t]
            for o in range(HALF // 8):
                part = pl.ds(pl.multiple_of(j * HALF + o * 8, 8), 8)
                a, b = got[t, part, :], got[t4, part, :]
                for h, pair in enumerate(
                    (jnp.where(lane < 64, a, pltpu.roll(b, 64, 1)), jnp.where(lane < 64, pltpu.roll(a, 64, 1), b))
                ):
                    at = h * HALF + o * 8
                    total = total + pair
                    rows[t, pl.ds(at, 8), :] = pair
                    for g in range(4):
                        cols[t, pl.ds(g * PITCH + at, 8), :] = take(pair, col_index[g])
            sums[t] = total
            return 0

        lax.fori_loop(0, 32, one, 0)

    def turn_field(target, r, f):
        row = spread(rows[r, pl.ds(f, 1), :])
        for q in range(2):
            target[f, q] = take(row, row_index[q])

    def work(i, now, later):
        _, tile = tile_at(i)
        r = first_block(tile)
        follow = first_block(tile_at(lax.rem(i + 1, TILES))[1])
        partner = [lax.rem(r + offset + s, 32) for s in range(4)]
        total = [[acc[tile, a // 16, a % 16]] for a in range(32)]
        for f in range(NF):
            turned = [now[f, q] for q in range(2)]
            for s in range(4):
                for g in range(4):
                    other = spread(cols[partner[s], pl.ds(g * PITCH + f, 1), :])
                    for q in range(2):
                        a = (g % 2) * 16 + (g // 2) * 8 + s * 2 + q
                        total[a][0] = total[a][0] + jnp.minimum(turned[q], other)
            turn_field(later, follow, f)
        for a in range(32):
            acc[tile, a // 16, a % 16] = total[a][0]

    def ready(j):
        def wait_one(i, _):
            a_copy(j, lax.rem(i * 13, 32)).wait_recv()
            return 0

        lax.fori_loop(1, 32, wait_one, 0)
        arrange(j)
        r0 = first_block(tile_at(0)[1])

        def first(b, _):
            for f in range(8):
                turn_field(roll_a, r0, b * 8 + f)
            return 0

        lax.fori_loop(0, NF // 8, first, 0)

    def round_of(j, _):
        ready(j)

        def two(i, _):
            work(2 * i, roll_a, roll_b)
            work(2 * i + 1, roll_b, roll_a)
            return 0

        lax.fori_loop(0, TILES // 2, two, 0)
        return 0

    lax.fori_loop(0, ROUNDS - 1, round_of, 0)

    ready(ROUNDS - 1)

    def total_one(t, _):
        turn[pl.ds(t, 1), :] = jnp.sum(sums[t], axis=0, keepdims=True)
        return 0

    lax.fori_loop(0, 32, total_one, 0)

    def pack_sums(tile, _):
        r = first_block(tile)
        packed = spread(turn[pl.ds(r, 1), :])
        for s in range(4):
            packed = jnp.where(sub == s + 1, spread(turn[pl.ds(lax.rem(r + offset + s, 32), 1), :]), packed)
        for c in range(2):
            acc[tile, c, 16] = packed
        return 0

    lax.fori_loop(0, TILES, pack_sums, 0)

    def core_copy(i):
        _, tile = tile_at(i)
        return pltpu.make_async_remote_copy(
            src_ref=acc.at[tile, 1 - core],
            dst_ref=core_in.at[tile],
            send_sem=c_send.at[i],
            recv_sem=c_recv.at[i],
            device_id=other_core,
            device_id_type=MESH,
        )

    def plane_copy(i):
        e, tile = tile_at(i)
        return pltpu.make_async_remote_copy(
            src_ref=acc.at[tile, core],
            dst_ref=plane_in.at[i],
            send_sem=p_send.at[i],
            recv_sem=p_recv.at[i],
            device_id=plane_peer(e),
            device_id_type=MESH,
        )

    def join_cores(i):
        _, tile = tile_at(i)
        core_copy(i).wait_recv()
        for a in range(17):
            acc[tile, core, a] = acc[tile, core, a] + core_in[tile, a]

    def last_two(i, _):
        work(2 * i, roll_a, roll_b)
        core_copy(2 * i).start()
        work(2 * i + 1, roll_b, roll_a)
        core_copy(2 * i + 1).start()

        @pl.when(i > 0)
        def _():
            for k in (2 * i - 2, 2 * i - 1):
                join_cores(k)
                plane_copy(k).start()

        return 0

    lax.fori_loop(0, TILES // 2, last_two, 0)
    join_cores(TILES - 2)
    plane_copy(TILES - 2).start()
    join_cores(TILES - 1)

    own = z * 4 + x
    whole = [acc[own, core, a] for a in range(17)]
    for i in range(TILES - 1):
        plane_copy(i).wait_recv()
        for a in range(17):
            whole[a] = whole[a] + plane_in[i, a]
    for half in range(2):
        for a in range(8):
            column_out[half, a] = whole[half * 8 + a]
        column_out[half, 8] = whole[16]

    def column_copy(d):
        y = lax.rem(column + d, 4)
        return pltpu.make_async_remote_copy(
            src_ref=column_out.at[lax.rem(y, 2)],
            dst_ref=column_in.at[d - 1],
            send_sem=y_send.at[d - 1],
            recv_sem=y_recv.at[d - 1],
            device_id=column_peer(d),
            device_id_type=MESH,
        )

    for d in (2, 1, 3):
        column_copy(d).start()
    whole = [column_out[yl, a] for a in range(9)]
    for d in (1, 3, 2):
        column_copy(d).wait_recv()
        for a in range(9):
            whole[a] = whole[a] + column_in[d - 1, a]

    turn[pl.ds(0, 8), :] = whole[8]
    mine = spread(turn[pl.ds(0, 1), :])
    own_sums = [take(mine, row_index[q]) for q in range(2)]
    group = yl * 2 + core
    for s in range(4):
        theirs = take(spread(turn[pl.ds(1 + s, 1), :]), lane_h * 64 + group * 16 + lane_c)
        for q in range(2):
            metric = 2.0 * whole[s * 2 + q] / (own_sums[q] + theirs)
            undo = ((lane_c - (sub + 8 * q)) % 16) * 8 + lane % 8
            xin[pl.ds((s * 2 + q) * 8, 8), pl.ds(0, 128)] = take(metric, undo)
    flat = xin[:, pl.ds(0, 128)]
    turned = jnp.concatenate([flat, flat], axis=0).T
    for i in range(16):
        index = (lane // 16) * 16 + (i - lane % 16) % 16
        turn[pl.ds(i * 8, 8), :] = take(turned[i * 8 : i * 8 + 8, :], index)
    for rho in range(4):
        out[pl.ds(rho * 16, 16), :] = turn[pl.ds(rho * 2 + yh, 16, stride=8), :]

    def finish(i, _):
        core_copy(i).wait_send()
        return 0

    lax.fori_loop(0, TILES, finish, 0)

    def finish_plane(i, _):
        plane_copy(i).wait_send()
        return 0

    lax.fori_loop(0, TILES - 1, finish_plane, 0)

    def finish_round(j, _):
        def finish_one(i, _):
            a_copy(j, lax.rem(i * 13, 32)).wait_send()
            return 0

        lax.fori_loop(1, 32, finish_one, 0)
        return 0

    lax.fori_loop(0, ROUNDS, finish_round, 0)
    for d in (1, 2, 3):
        column_copy(d).wait_send()


def per_device(vectors, section):
    f32 = jnp.float32
    dma = pltpu.SemaphoreType.DMA
    flat = pl.pallas_call(
        kernel,
        out_shape=jax.ShapeDtypeStruct((64, 128), f32),
        in_specs=[pl.BlockSpec(memory_space=pltpu.SMEM), pl.BlockSpec(memory_space=pl.ANY)],
        out_specs=pl.BlockSpec(memory_space=pltpu.VMEM),
        scratch_shapes=[
            pltpu.VMEM((64, 8192), f32),
            pltpu.VMEM((32, 128, 128), f32),
            pltpu.VMEM((32, 128, 128), f32),
            pltpu.VMEM((32, NF, 128), f32),
            pltpu.VMEM((32, 4 * PITCH, 128), f32),
            pltpu.VMEM((NF, 2, 8, 128), f32),
            pltpu.VMEM((NF, 2, 8, 128), f32),
            pltpu.VMEM((TILES, 2, 17, 8, 128), f32),
            pltpu.VMEM((32, 8, 128), f32),
            pltpu.VMEM((TILES, 17, 8, 128), f32),
            pltpu.VMEM((TILES, 17, 8, 128), f32),
            pltpu.VMEM((2, 9, 8, 128), f32),
            pltpu.VMEM((3, 9, 8, 128), f32),
            pltpu.VMEM((128, 128), f32),
            dma((8,)),
            dma((ROUNDS, 32)),
            dma((ROUNDS, 32)),
            dma((TILES,)),
            dma((TILES,)),
            dma((TILES,)),
            dma((TILES,)),
            dma((3,)),
            dma((3,)),
        ],
        compiler_params=pltpu.CompilerParams(
            collective_id=0, has_side_effects=True, vmem_limit_bytes=48 * 2**20
        ),
    )(section, vectors)
    return flat[:, :64].reshape(64, 4, 16)


def solution(mesh):
    torus = Mesh(mesh.devices.reshape(4, 2, 4, 2, 2), AXES)
    placed = (P(("z", "yh", "x"), ("yl", "core")), P())
    return jax.shard_map(
        per_device,
        mesh=torus,
        in_specs=placed,
        out_specs=P(("z", "yh", "x"), None, ("yl", "core")),
        check_vma=False,
    )
```

```python
import jax
import jax.numpy as jnp
from jax import lax
from jax.experimental import pallas as pl
from jax.experimental.pallas import tpu as pltpu
from jax.sharding import Mesh
from jax.sharding import PartitionSpec as P

MESH = pl.DeviceIdType.MESH
AXES = ("z", "yh", "x", "yl", "core")
FIELDS = (32, 64, 64, 96)
ROUNDS = len(FIELDS)
START = [sum(FIELDS[:j]) // 2 for j in range(ROUNDS)]
MOST = max(FIELDS)
TILES = 16
VREG = (8, 128)


def iota(axis):
    return lax.broadcasted_iota(jnp.int32, VREG, axis)


def spread(row):
    return jnp.broadcast_to(row, VREG)


def take(value, index):
    return jnp.take_along_axis(value, index, axis=1)


def kernel(
    section, x_hbm, out, xin, sent, got, places, high, low, rows, cols, roll_a, roll_b, acc, sums, core_in, plane_in, column_out, column_in,
    turn, flat_out, load_sem, a_send, a_recv, c_send, c_recv, p_send, p_recv, y_send, y_recv,
):
    z, yh, x, yl, core = (lax.axis_index(name) for name in AXES)
    offset = section[0]
    block = z * 8 + yh * 4 + x
    column = yh * 2 + yl

    def blk_peer(e):
        return (lax.rem(z + e // 8, 4), lax.rem(yh + (e // 4) % 2, 2), lax.rem(x + e % 4, 4), yl, core)

    def plane_peer(e):
        return (lax.rem(z + e // 4, 4), yh, lax.rem(x + e % 4, 4), yl, core)

    def column_peer(d):
        y = lax.rem(column + d, 4)
        return (z, y // 2, x, lax.rem(y, 2), core)

    other_core = (z, yh, x, yl, 1 - core)

    loads = []
    for i in range(8):
        part = pl.ds(i * 1024, 1024)
        loads.append(pltpu.make_async_copy(x_hbm.at[:, part], xin.at[:, part], load_sem.at[i]))
        loads[-1].start()

    barrier = pltpu.get_barrier_semaphore()
    for e in range(1, 32):
        pl.semaphore_signal(barrier, inc=1, device_id=blk_peer(e), device_id_type=MESH)
    for peer in (column_peer(1), column_peer(3), other_core):
        pl.semaphore_signal(barrier, inc=1, device_id=peer, device_id_type=MESH)

    lane, sub = iota(1), iota(0)
    lane_c = lane // 8

    with jax.named_scope("load_wait"):
        for load in loads:
            load.wait()

    def transpose_some(n, _):
        for k in range(8):
            u = n * 8 + k
            left = xin[:, pl.ds(pl.multiple_of(u * 128, 128), 128)]
            right = xin[:, pl.ds(pl.multiple_of(u * 128 + 4096, 128), 128)]
            sent[u] = jnp.concatenate([left, right], axis=0).T
        return 0

    with jax.named_scope("transpose"):
        lax.fori_loop(0, 4, transpose_some, 0)
        got[block] = sent[block]
    for tile in range(32):
        sums[tile] = jnp.zeros(VREG, jnp.float32)

    def clear(tile, _):
        for c in range(2):
            for a in range(16):
                acc[tile, c, a] = jnp.zeros(VREG, jnp.float32)
        return 0

    with jax.named_scope("clear"):
        lax.fori_loop(0, TILES, clear, 0)
    with jax.named_scope("barrier"):
        pl.semaphore_wait(barrier, 34)

    def a_copy(j, e):
        z2, yh2, x2, _, _ = blk_peer(e)
        part = pl.ds(START[j], FIELDS[j] // 2)
        return pltpu.make_async_remote_copy(
            src_ref=sent.at[z2 * 8 + yh2 * 4 + x2, part],
            dst_ref=got.at[block, part],
            send_sem=a_send.at[j, e],
            recv_sem=a_recv.at[j, e],
            device_id=blk_peer(e),
            device_id_type=MESH,
        )

    def over_peers(act):
        def one(i, _):
            act(lax.rem(i * 13, 32))
            return 0

        lax.fori_loop(1, 32, one, 0)

    with jax.named_scope("send"):
        for j in range(ROUNDS):
            over_peers(lambda e: a_copy(j, e).start())

    def tile_at(i):
        e = lax.rem((15 - i) * 7, 16)
        return e, lax.rem(z + e // 4, 4) * 4 + lax.rem(x + e % 4, 4)

    def first_block(tile):
        return (tile // 4) * 8 + lax.rem(tile, 4)

    def place():
        here = lax.broadcasted_iota(jnp.int32, (256, 128), 0)
        to = lax.broadcasted_iota(jnp.int32, (256, 128), 1)
        for order in range(5):
            group = (to // 2) % 4 if order == 0 else order - 1
            for h in range(2):
                origin = (to % 2) * 128 + h * 64 + group * 16 + to // 8
                part = pl.ds((order * 2 + h) * 128, 128)
                places[:, part] = jnp.where(here == origin, 1.0, 0.0).astype(jnp.bfloat16)

    def arrange(j):
        half = FIELDS[j] // 2
        pitch = FIELDS[j] + 8
        n = {16: 32, 32: 32, 48: 16}[half]

        def split(b, _):
            for k in range(4):
                t = b * 4 + k
                here = pl.ds(pl.multiple_of(t * half, 16), half)
                for i, source in enumerate((t, lax.rem(t + 4, 32))):
                    value = got[source, pl.ds(START[j], half), :]
                    top = value.astype(jnp.bfloat16)
                    high[here, pl.ds(i * 128, 128)] = top
                    low[here, pl.ds(i * 128, 128)] = (value - top.astype(jnp.float32)).astype(jnp.bfloat16)
            return 0

        def spread_out(b, _):
            here = pl.ds(pl.multiple_of(b * n * half, 16), n * half)
            for order in range(5):
                weight = places[:, pl.ds(order * 256, 256)]
                value = jnp.dot(high[here, :], weight, preferred_element_type=jnp.float32)
                value = value + jnp.dot(low[here, :], weight, preferred_element_type=jnp.float32)
                for k in range(n):
                    for h in range(2):
                        part = value[k * half : (k + 1) * half, h * 128 : h * 128 + 128]
                        if order == 0:
                            rows[b * n + k, pl.ds(h * half, half), :] = part
                        else:
                            cols[b * n + k, pl.ds((order - 1) * pitch + h * half, half), :] = part
            return 0

        def add_up(b, _):
            for k in range(4):
                total = sums[b * 4 + k]
                for o in range(FIELDS[j] // 8):
                    total = total + rows[b * 4 + k, pl.ds(o * 8, 8), :]
                sums[b * 4 + k] = total
            return 0

        lax.fori_loop(0, 8, split, 0)
        lax.fori_loop(0, 32 // n, spread_out, 0)
        lax.fori_loop(0, 8, add_up, 0)

    def turn_field(j, target, r, f):
        row = spread(rows[r, pl.ds(f, 1), :])
        for q in range(2):
            target[f, q] = pltpu.roll(row, 64 * q, 1, stride=8, stride_axis=0)

    def work(j, i, now, later):
        _, tile = tile_at(i)
        r = first_block(tile)
        follow = first_block(tile_at(lax.rem(i + 1, TILES))[1])
        partner = [lax.rem(r + offset + s, 32) for s in range(4)]
        total = [acc[tile, a // 16, a % 16] for a in range(32)]
        for f in range(FIELDS[j]):
            turned = [now[f, q] for q in range(2)]
            for s in range(4):
                for g in range(4):
                    other = spread(cols[partner[s], pl.ds(g * (FIELDS[j] + 8) + f, 1), :])
                    for q in range(2):
                        a = (g % 2) * 16 + (g // 2) * 8 + s * 2 + q
                        total[a] = total[a] + jnp.minimum(turned[q], other)
            turn_field(j, later, follow, f)
        for a in range(32):
            acc[tile, a // 16, a % 16] = total[a]

    def first_turn(j):
        r0 = first_block(tile_at(0)[1])

        def some(b, _):
            for f in range(16):
                turn_field(j, roll_a, r0, b * 16 + f)
            return 0

        with jax.named_scope("first"):
            lax.fori_loop(0, FIELDS[j] // 16, some, 0)

    def arrived(j):
        with jax.named_scope("got_wait"):
            over_peers(lambda e: a_copy(j, e).wait_recv())

    def ready(j):
        arrived(j)
        with jax.named_scope("arrange"):
            arrange(j)
        first_turn(j)

    def round_of(j):
        ready(j)

        def two(i, _):
            work(j, 2 * i, roll_a, roll_b)

            @pl.when(i < TILES)
            def _():
                work(j, 2 * i + 1, roll_b, roll_a)

            return 0

        with jax.named_scope("work"):
            lax.fori_loop(0, TILES // 2, two, 0)

    with jax.named_scope("place"):
        place()
    for j in range(ROUNDS - 1):
        round_of(j)
    ready(ROUNDS - 1)

    def total_one(t, _):
        turn[pl.ds(t, 1), :] = jnp.sum(sums[t], axis=0, keepdims=True)
        return 0

    with jax.named_scope("total"):
        lax.fori_loop(0, 32, total_one, 0)

    def pack_sums(tile, _):
        r = first_block(tile)
        packed = spread(turn[pl.ds(r, 1), :])
        for s in range(4):
            packed = jnp.where(sub == s + 1, spread(turn[pl.ds(lax.rem(r + offset + s, 32), 1), :]), packed)
        for c in range(2):
            acc[tile, c, 16] = packed
        return 0

    with jax.named_scope("pack"):
        lax.fori_loop(0, TILES, pack_sums, 0)

    def core_copy(i):
        _, tile = tile_at(i)
        return pltpu.make_async_remote_copy(
            src_ref=acc.at[tile, 1 - core],
            dst_ref=core_in.at[tile],
            send_sem=c_send.at[i],
            recv_sem=c_recv.at[i],
            device_id=other_core,
            device_id_type=MESH,
        )

    def plane_copy(i):
        e, tile = tile_at(i)
        return pltpu.make_async_remote_copy(
            src_ref=acc.at[tile, core],
            dst_ref=plane_in.at[i],
            send_sem=p_send.at[i],
            recv_sem=p_recv.at[i],
            device_id=plane_peer(e),
            device_id_type=MESH,
        )

    def join_cores(i):
        _, tile = tile_at(i)
        core_copy(i).wait_recv()
        for a in range(17):
            acc[tile, core, a] = acc[tile, core, a] + core_in[tile, a]

    def last_two(i, _):
        work(ROUNDS - 1, 2 * i, roll_a, roll_b)
        core_copy(2 * i).start()
        work(ROUNDS - 1, 2 * i + 1, roll_b, roll_a)
        core_copy(2 * i + 1).start()

        @pl.when(i > 0)
        def _():
            for k in (2 * i - 2, 2 * i - 1):
                join_cores(k)
                plane_copy(k).start()

        return 0

    with jax.named_scope("last_work"):
        lax.fori_loop(0, TILES // 2, last_two, 0)
    with jax.named_scope("last_join"):
        join_cores(TILES - 2)
        plane_copy(TILES - 2).start()
        join_cores(TILES - 1)

    with jax.named_scope("finish"):
        for j in range(ROUNDS):
            over_peers(lambda e: a_copy(j, e).wait_send())
    own = z * 4 + x
    whole = [acc[own, core, a] for a in range(17)]
    for i in range(TILES - 1):
        with jax.named_scope("plane_wait"):
            plane_copy(i).wait_recv()
        for a in range(17):
            whole[a] = whole[a] + plane_in[i, a]
    for half in range(2):
        for a in range(8):
            column_out[half, a] = whole[half * 8 + a]
        column_out[half, 8] = whole[16]

    def column_copy(d):
        y = lax.rem(column + d, 4)
        return pltpu.make_async_remote_copy(
            src_ref=column_out.at[lax.rem(y, 2)],
            dst_ref=column_in.at[d - 1],
            send_sem=y_send.at[d - 1],
            recv_sem=y_recv.at[d - 1],
            device_id=column_peer(d),
            device_id_type=MESH,
        )

    for d in (2, 1, 3):
        column_copy(d).start()

    def finish(i, _):
        core_copy(i).wait_send()
        return 0

    def finish_plane(i, _):
        plane_copy(i).wait_send()
        return 0

    lax.fori_loop(0, TILES, finish, 0)
    lax.fori_loop(0, TILES - 1, finish_plane, 0)
    whole = [column_out[yl, a] for a in range(9)]
    for d in (1, 3, 2):
        with jax.named_scope("column_wait"):
            column_copy(d).wait_recv()
        column_copy(d).wait_send()
        for a in range(9):
            whole[a] = whole[a] + column_in[d - 1, a]

    with jax.named_scope("end"):
        turn[pl.ds(0, 8), :] = whole[8]
        mine = spread(turn[pl.ds(0, 1), :])
        pick = lane_c * 8 + (yl * 2 + core) * 2 + lane % 2
        theirs = [take(spread(turn[pl.ds(1 + s, 1), :]), pick) for s in range(4)]
        for q in range(2):
            own_sums = pltpu.roll(mine, 64 * q, 1, stride=8, stride_axis=0)
            undo = ((lane_c + sub + 8 * q) % 16) * 8 + lane % 8
            for s in range(4):
                metric = 2.0 * whole[s * 2 + q] / (own_sums + theirs[s])
                flat_out[pl.ds(q * 32 + s, 8, stride=4), :] = take(metric, undo)
        flat = flat_out[...]
        turned = jnp.concatenate([flat, flat], axis=0).T
        for i in range(16):
            part = turned[i * 8 : i * 8 + 8, :]
            turn[pl.ds(i * 8, 8), :] = pltpu.roll(part, 4 * i, 1) if i else part
        swap = (lane % 16) * 4 + lane // 16
        for i in range(8):
            part = turn[pl.ds((i % 2) * 64 + (i // 2) * 2 + yh, 8, stride=8), :]
            out[pl.ds(i * 8, 8), :] = take(part, swap % 128)


def per_device(vectors, section):
    f32 = jnp.float32
    dma = pltpu.SemaphoreType.DMA
    flat = pl.pallas_call(
        kernel,
        out_shape=jax.ShapeDtypeStruct((64, 128), f32),
        in_specs=[pl.BlockSpec(memory_space=pltpu.SMEM), pl.BlockSpec(memory_space=pl.ANY)],
        out_specs=pl.BlockSpec(memory_space=pltpu.VMEM),
        scratch_shapes=[
            pltpu.VMEM((64, 8192), f32),
            pltpu.VMEM((32, 128, 128), f32),
            pltpu.VMEM((32, 128, 128), f32),
            pltpu.VMEM((256, 1280), jnp.bfloat16),
            pltpu.VMEM((16 * MOST, 256), jnp.bfloat16),
            pltpu.VMEM((16 * MOST, 256), jnp.bfloat16),
            pltpu.VMEM((32, MOST, 128), f32),
            pltpu.VMEM((32, 4 * (MOST + 8), 128), f32),
            pltpu.VMEM((MOST, 2, 8, 128), f32),
            pltpu.VMEM((MOST, 2, 8, 128), f32),
            pltpu.VMEM((TILES, 2, 17, 8, 128), f32),
            pltpu.VMEM((32, 8, 128), f32),
            pltpu.VMEM((TILES, 17, 8, 128), f32),
            pltpu.VMEM((TILES, 17, 8, 128), f32),
            pltpu.VMEM((2, 9, 8, 128), f32),
            pltpu.VMEM((3, 9, 8, 128), f32),
            pltpu.VMEM((128, 128), f32),
            pltpu.VMEM((64, 128), f32),
            dma((8,)),
            dma((ROUNDS, 32)),
            dma((ROUNDS, 32)),
            dma((TILES,)),
            dma((TILES,)),
            dma((TILES,)),
            dma((TILES,)),
            dma((3,)),
            dma((3,)),
        ],
        compiler_params=pltpu.CompilerParams(
            collective_id=0, has_side_effects=True, vmem_limit_bytes=63 * 2**20
        ),
    )(section, vectors)
    return flat[:, :64].reshape(64, 4, 16)


def solution(mesh):
    torus = Mesh(mesh.devices.reshape(4, 2, 4, 2, 2), AXES)
    placed = (P(("z", "yh", "x"), ("yl", "core")), P())
    return jax.shard_map(
        per_device,
        mesh=torus,
        in_specs=placed,
        out_specs=P(("z", "yh", "x"), None, ("yl", "core")),
        check_vma=False,
    )
```

```python
import jax
import jax.numpy as jnp
from jax import lax
from jax.experimental import pallas as pl
from jax.experimental.pallas import tpu as pltpu
from jax.sharding import Mesh
from jax.sharding import PartitionSpec as P

MESH = pl.DeviceIdType.MESH


def hops(e):
    return min(e // 8, 4 - e // 8) + 2 * ((e // 4) % 2) + min(e % 4, 4 - e % 4)


FAR_FIRST = sorted(range(1, 32), key=lambda e: (-hops(e), (e * 13) % 32))
AXES = ("z", "yh", "x", "yl", "core")
FIELDS = (32, 64, 32, 128)
ROUNDS = len(FIELDS)
START = [sum(FIELDS[:j]) // 2 for j in range(ROUNDS)]
MOST = max(FIELDS)
TILES = 16
ORDER = (10, 9, 11, 6, 14, 5, 7, 13, 15, 2, 8, 1, 12, 3, 4, 0)
VREG = (8, 128)


def iota(axis):
    return lax.broadcasted_iota(jnp.int32, VREG, axis)


def spread(row):
    return jnp.broadcast_to(row, VREG)


def take(value, index):
    return jnp.take_along_axis(value, index, axis=1)


def kernel(
    section, x_hbm, out, xin, sent, got, places, high, low, rows, cols, roll_a, roll_b, acc, sums, core_in, plane_in, column_out, column_in,
    turn, flat_out, load_sem, a_send, a_recv, c_send, c_recv, p_send, p_recv, y_send, y_recv,
):
    z, yh, x, yl, core = (lax.axis_index(name) for name in AXES)
    offset = section[0]
    block = z * 8 + yh * 4 + x
    column = yh * 2 + yl

    def blk_peer(e):
        return (lax.rem(z + e // 8, 4), lax.rem(yh + (e // 4) % 2, 2), lax.rem(x + e % 4, 4), yl, core)

    def plane_peer(e):
        return (lax.rem(z + e // 4, 4), yh, lax.rem(x + e % 4, 4), yl, core)

    def column_peer(d):
        y = lax.rem(column + d, 4)
        return (z, y // 2, x, lax.rem(y, 2), core)

    other_core = (z, yh, x, yl, 1 - core)

    loads = []
    for i in range(8):
        part = pl.ds(i * 1024, 1024)
        loads.append(pltpu.make_async_copy(x_hbm.at[:, part], xin.at[:, part], load_sem))
        loads[-1].start()

    barrier = pltpu.get_barrier_semaphore()
    for e in FAR_FIRST:
        pl.semaphore_signal(barrier, inc=1, device_id=blk_peer(e), device_id_type=MESH)
    for peer in (column_peer(1), column_peer(3), other_core):
        pl.semaphore_signal(barrier, inc=1, device_id=peer, device_id_type=MESH)

    lane, sub = iota(1), iota(0)
    lane_c = lane // 8

    with jax.named_scope("load_wait"):
        pltpu.make_async_copy(x_hbm, xin, load_sem).wait()

    def transpose_some(n, _):
        for k in range(8):
            u = n * 8 + k
            left = xin[:, pl.ds(pl.multiple_of(u * 128, 128), 128)]
            right = xin[:, pl.ds(pl.multiple_of(u * 128 + 4096, 128), 128)]
            sent[u] = jnp.concatenate([left, right], axis=0).T
        return 0

    with jax.named_scope("transpose"):
        lax.fori_loop(0, 4, transpose_some, 0)
        got[block] = sent[block]
    for tile in range(32):
        sums[tile] = jnp.zeros(VREG, jnp.float32)

    def clear(tile, _):
        for c in range(2):
            for a in range(16):
                acc[tile, c, a] = jnp.zeros(VREG, jnp.float32)
        return 0

    with jax.named_scope("barrier"):
        pl.semaphore_wait(barrier, 34)

    def a_copy(j, e):
        z2, yh2, x2, _, _ = blk_peer(e)
        part = pl.ds(START[j], FIELDS[j] // 2)
        return pltpu.make_async_remote_copy(
            src_ref=sent.at[z2 * 8 + yh2 * 4 + x2, part],
            dst_ref=got.at[block, part],
            send_sem=a_send,
            recv_sem=a_recv.at[j],
            device_id=blk_peer(e),
            device_id_type=MESH,
        )

    def over_peers(act):
        def one(i, _):
            act(lax.rem(i * 13, 32))
            return 0

        lax.fori_loop(1, 32, one, 0)

    with jax.named_scope("send"):
        for e in FAR_FIRST:
            a_copy(0, e).start()
        for j in range(1, ROUNDS):
            over_peers(lambda e: a_copy(j, e).start())

    def tile_at(i, last=True):
        e = sum(jnp.where(i == k, ORDER[k], 0) for k in range(TILES)) if last else i
        return e, lax.rem(z + e // 4, 4) * 4 + lax.rem(x + e % 4, 4)

    def first_block(tile):
        return (tile // 4) * 8 + lax.rem(tile, 4)

    def place():
        here = lax.broadcasted_iota(jnp.int32, (256, 128), 0)
        to = lax.broadcasted_iota(jnp.int32, (256, 128), 1)
        for order in range(5):
            group = (to // 2) % 4 if order == 0 else order - 1
            for h in range(2):
                origin = (to % 2) * 128 + h * 64 + group * 16 + to // 8
                part = pl.ds((order * 2 + h) * 128, 128)
                places[:, part] = jnp.where(here == origin, 1.0, 0.0).astype(jnp.bfloat16)

    def arrange(j):
        half = FIELDS[j] // 2
        pitch = FIELDS[j] + 8
        n = min(32, 1024 // half)

        def split(b, _):
            for k in range(8):
                t = b * 8 + k
                value = got[t, pl.ds(START[j], half), :]
                top = value.astype(jnp.bfloat16)
                rest = (value - top.astype(jnp.float32)).astype(jnp.bfloat16)
                for i, target in enumerate((t, lax.rem(t + 28, 32))):
                    here = pl.ds(pl.multiple_of(target * half, 16), half)
                    high[here, pl.ds(i * 128, 128)] = top
                    low[here, pl.ds(i * 128, 128)] = rest
                total = sums[t]
                for o in range(half // 8):
                    total = total + value[o * 8 : o * 8 + 8]
                sums[t] = total
            return 0

        def spread_out(b, _):
            here = pl.ds(pl.multiple_of(b * n * half, 16), n * half)
            for order in range(5):
                weight = places[:, pl.ds(order * 256, 256)]
                value = jnp.dot(high[here, :], weight, preferred_element_type=jnp.float32)
                value = value + jnp.dot(low[here, :], weight, preferred_element_type=jnp.float32)
                for k in range(n):
                    for h in range(2):
                        part = value[k * half : (k + 1) * half, h * 128 : h * 128 + 128]
                        if order == 0:
                            rows[b * n + k, pl.ds(h * half, half), :] = part
                        else:
                            cols[b * n + k, pl.ds((order - 1) * pitch + h * half, half), :] = part
            return 0

        lax.fori_loop(0, 4, split, 0)
        lax.fori_loop(0, 32 // n, spread_out, 0)

    def turn_field(j, target, r, f):
        row = spread(rows[r, pl.ds(f, 1), :])
        for q in range(2):
            target[f, q] = pltpu.roll(row, 64 * q, 1, stride=8, stride_axis=0)

    def work(j, i, now, later):
        last = j == ROUNDS - 1
        _, tile = tile_at(i, last)
        r = first_block(tile)
        follow = first_block(tile_at(lax.rem(i + 1, TILES), last)[1])
        partner = [lax.rem(r + offset + s, 32) for s in range(4)]
        total = [acc[tile, a // 16, a % 16] for a in range(32)]
        for f in range(FIELDS[j]):
            turned = [now[f, q] for q in range(2)]
            for s in range(4):
                for g in range(4):
                    other = spread(cols[partner[s], pl.ds(g * (FIELDS[j] + 8) + f, 1), :])
                    for q in range(2):
                        a = (g % 2) * 16 + (g // 2) * 8 + s * 2 + q
                        total[a] = total[a] + jnp.minimum(turned[q], other)
            turn_field(j, later, follow, f)
        for a in range(32):
            acc[tile, a // 16, a % 16] = total[a]

    def first_turn(j):
        r0 = first_block(tile_at(0, j == ROUNDS - 1)[1])

        def some(b, _):
            for f in range(32):
                turn_field(j, roll_a, r0, b * 32 + f)
            return 0

        with jax.named_scope("first"):
            lax.fori_loop(0, FIELDS[j] // 32, some, 0)

    def arrived(j):
        with jax.named_scope("got_wait"):
            part = pl.ds(START[j], FIELDS[j] // 2)
            pltpu.make_async_copy(sent.at[pl.ds(0, 31), part], got.at[pl.ds(0, 31), part], a_recv.at[j]).wait()

    def ready(j):
        arrived(j)
        with jax.named_scope("arrange"):
            arrange(j)
        first_turn(j)

    def round_of(j):
        ready(j)

        def two(i, _):
            work(j, 2 * i, roll_a, roll_b)

            @pl.when(i < TILES)
            def _():
                work(j, 2 * i + 1, roll_b, roll_a)

            return 0

        with jax.named_scope("work"):
            lax.fori_loop(0, TILES // 2, two, 0)

    with jax.named_scope("place"):
        place()
        lax.fori_loop(0, TILES, clear, 0)
    for j in range(ROUNDS - 1):
        round_of(j)
    ready(ROUNDS - 1)

    def total_one(b, _):
        for k in range(8):
            turn[pl.ds(b * 8 + k, 1), :] = jnp.sum(sums[b * 8 + k], axis=0, keepdims=True)
        return 0

    with jax.named_scope("total"):
        lax.fori_loop(0, 4, total_one, 0)
        natural = turn[pl.ds(0, 32), :]
        natural = jnp.concatenate([natural, jnp.concatenate([natural[4:], natural[:4]], axis=0)], axis=1)
        top = natural.astype(jnp.bfloat16)
        rest = (natural - top.astype(jnp.float32)).astype(jnp.bfloat16)
        weight = places[:, pl.ds(0, 256)]
        both = jnp.dot(top, weight, preferred_element_type=jnp.float32)
        both = both + jnp.dot(rest, weight, preferred_element_type=jnp.float32)
        turn[pl.ds(0, 32), :] = both[:, :128] + both[:, 128:]

    def pack_sums(tile, _):
        r = first_block(tile)
        packed = spread(turn[pl.ds(r, 1), :])
        for s in range(4):
            packed = jnp.where(sub == s + 1, spread(turn[pl.ds(lax.rem(r + offset + s, 32), 1), :]), packed)
        for c in range(2):
            acc[tile, c, 16] = packed
        return 0

    with jax.named_scope("pack"):
        lax.fori_loop(0, TILES, pack_sums, 0)

    def core_copy(i):
        _, tile = tile_at(i)
        return pltpu.make_async_remote_copy(
            src_ref=acc.at[tile, 1 - core],
            dst_ref=core_in.at[tile],
            send_sem=c_send,
            recv_sem=c_recv.at[i],
            device_id=other_core,
            device_id_type=MESH,
        )

    def plane_copy(i):
        e, tile = tile_at(i)
        return pltpu.make_async_remote_copy(
            src_ref=acc.at[tile, core],
            dst_ref=plane_in.at[i],
            send_sem=p_send,
            recv_sem=p_recv,
            device_id=plane_peer(e),
            device_id_type=MESH,
        )

    def join_cores(i):
        _, tile = tile_at(i)
        core_copy(i).wait_recv()
        for a in range(17):
            acc[tile, core, a] = acc[tile, core, a] + core_in[tile, a]

    def last_two(i, _):
        work(ROUNDS - 1, 2 * i, roll_a, roll_b)
        core_copy(2 * i).start()
        work(ROUNDS - 1, 2 * i + 1, roll_b, roll_a)
        core_copy(2 * i + 1).start()

        @pl.when(i > 0)
        def _():
            for k in (2 * i - 2, 2 * i - 1):
                join_cores(k)
                plane_copy(k).start()

        return 0

    with jax.named_scope("last_work"):
        lax.fori_loop(0, TILES // 2, last_two, 0)
    with jax.named_scope("last_join"):
        join_cores(TILES - 2)
        plane_copy(TILES - 2).start()
        join_cores(TILES - 1)

    with jax.named_scope("finish"):
        pltpu.make_async_copy(got.at[pl.ds(0, 31)], sent.at[pl.ds(0, 31)], a_send).wait()
    own = z * 4 + x
    whole = [acc[own, core, a] for a in range(17)]
    with jax.named_scope("plane_wait"):
        pltpu.make_async_copy(acc.at[pl.ds(0, 15), 0], plane_in.at[pl.ds(0, 15)], p_recv).wait()
    for i in range(TILES - 1):
        for a in range(17):
            whole[a] = whole[a] + plane_in[i, a]
    for half in range(2):
        for a in range(8):
            column_out[half, a] = whole[half * 8 + a]
        column_out[half, 8] = whole[16]

    def column_copy(d):
        y = lax.rem(column + d, 4)
        return pltpu.make_async_remote_copy(
            src_ref=column_out.at[lax.rem(y, 2)],
            dst_ref=column_in.at[d - 1],
            send_sem=y_send,
            recv_sem=y_recv,
            device_id=column_peer(d),
            device_id_type=MESH,
        )

    for d in (2, 1, 3):
        column_copy(d).start()

    pltpu.make_async_copy(acc.at[:, 0], core_in, c_send).wait()
    pltpu.make_async_copy(acc.at[pl.ds(0, 15), 0], plane_in.at[pl.ds(0, 15)], p_send).wait()
    whole = [column_out[yl, a] for a in range(9)]
    with jax.named_scope("column_wait"):
        pltpu.make_async_copy(column_in, column_in, y_recv).wait()
        pltpu.make_async_copy(column_in, column_in, y_send).wait()
    for d in range(3):
        for a in range(9):
            whole[a] = whole[a] + column_in[d, a]

    with jax.named_scope("end"):
        turn[pl.ds(0, 8), :] = whole[8]
        mine = spread(turn[pl.ds(0, 1), :])
        pick = lane_c * 8 + (yl * 2 + core) * 2 + lane % 2
        theirs = [take(spread(turn[pl.ds(1 + s, 1), :]), pick) for s in range(4)]
        for q in range(2):
            own_sums = pltpu.roll(mine, 64 * q, 1, stride=8, stride_axis=0)
            undo = ((lane_c + sub + 8 * q) % 16) * 8 + lane % 8
            for s in range(4):
                metric = 2.0 * whole[s * 2 + q] / (own_sums + theirs[s])
                flat_out[pl.ds(q * 32 + s, 8, stride=4), :] = take(metric, undo)
        flat = flat_out[pl.ds(0, 64), :]
        turned = jnp.concatenate([flat, flat], axis=0).T
        for i in range(16):
            part = turned[i * 8 : i * 8 + 8, :]
            turn[pl.ds(i * 8, 8), :] = pltpu.roll(part, 4 * i, 1) if i else part
        for i in range(8):
            part = turn[pl.ds((i % 2) * 64 + (i // 2) * 2 + yh, 8, stride=8), :]
            flat_out[pl.ds(i * 8, 8), :] = part
            flat_out[pl.ds(64 + i * 8, 8), :] = part
        turn[...] = flat_out[...].T
        for s in range(4):
            out[pl.ds(s * 16, 16), :] = turn[pl.ds(s, 16, stride=4), :]


def per_device(vectors, section):
    f32 = jnp.float32
    dma = pltpu.SemaphoreType.DMA
    flat = pl.pallas_call(
        kernel,
        out_shape=jax.ShapeDtypeStruct((64, 128), f32),
        in_specs=[pl.BlockSpec(memory_space=pltpu.SMEM), pl.BlockSpec(memory_space=pl.ANY)],
        out_specs=pl.BlockSpec(memory_space=pltpu.VMEM),
        scratch_shapes=[
            pltpu.VMEM((64, 8192), f32),
            pltpu.VMEM((32, 128, 128), f32),
            pltpu.VMEM((32, 128, 128), f32),
            pltpu.VMEM((256, 1280), jnp.bfloat16),
            pltpu.VMEM((16 * MOST, 256), jnp.bfloat16),
            pltpu.VMEM((16 * MOST, 256), jnp.bfloat16),
            pltpu.VMEM((32, MOST, 128), f32),
            pltpu.VMEM((32, 4 * (MOST + 8), 128), f32),
            pltpu.VMEM((MOST, 2, 8, 128), f32),
            pltpu.VMEM((MOST, 2, 8, 128), f32),
            pltpu.VMEM((TILES, 2, 17, 8, 128), f32),
            pltpu.VMEM((32, 8, 128), f32),
            pltpu.VMEM((TILES, 17, 8, 128), f32),
            pltpu.VMEM((TILES, 17, 8, 128), f32),
            pltpu.VMEM((2, 9, 8, 128), f32),
            pltpu.VMEM((3, 9, 8, 128), f32),
            pltpu.VMEM((128, 128), f32),
            pltpu.VMEM((128, 128), f32),
            dma,
            dma,
            dma((ROUNDS,)),
            dma,
            dma((TILES,)),
            dma,
            dma,
            dma,
            dma,
        ],
        compiler_params=pltpu.CompilerParams(
            collective_id=0, has_side_effects=True, vmem_limit_bytes=63 * 2**20
        ),
    )(section, vectors)
    return flat[:, :64].reshape(4, 16, 64).transpose(2, 0, 1)


def solution(mesh):
    torus = Mesh(mesh.devices.reshape(4, 2, 4, 2, 2), AXES)
    placed = (P(("z", "yh", "x"), ("yl", "core")), P())
    return jax.shard_map(
        per_device,
        mesh=torus,
        in_specs=placed,
        out_specs=P(("z", "yh", "x"), None, ("yl", "core")),
        check_vma=False,
    )
```

```python
import jax
import jax.numpy as jnp
from jax import lax
from jax.experimental import pallas as pl
from jax.experimental.pallas import tpu as pltpu
from jax.sharding import Mesh
from jax.sharding import PartitionSpec as P

MESH = pl.DeviceIdType.MESH


def hops(e):
    return min(e // 8, 4 - e // 8) + 2 * ((e // 4) % 2) + min(e % 4, 4 - e % 4)


FAR_FIRST = sorted(range(1, 32), key=lambda e: (-hops(e), (e * 13) % 32))
AXES = ("z", "yh", "x", "yl", "core")
FIELDS = (32, 64, 32, 128)
ROUNDS = len(FIELDS)
START = [sum(FIELDS[:j]) // 2 for j in range(ROUNDS)]
MOST = max(FIELDS)
TILES = 16
ORDER = (10, 9, 11, 6, 14, 5, 7, 13, 15, 2, 8, 1, 12, 3, 4, 0)
VREG = (8, 128)


def iota(axis):
    return lax.broadcasted_iota(jnp.int32, VREG, axis)


def spread(row):
    return jnp.broadcast_to(row, VREG)


def take(value, index):
    return jnp.take_along_axis(value, index, axis=1)


def kernel(
    section, x_hbm, out, xin, sent, got, places, near, cross, rows, cols, roll_a, roll_b, acc, sums, core_in, plane_in, column_out, column_in,
    turn, flat_out, load_sem, a_send, a_recv, c_send, c_recv, p_send, p_recv, y_send, y_recv,
):
    z, yh, x, yl, core = (lax.axis_index(name) for name in AXES)
    offset = section[0]
    block = z * 8 + yh * 4 + x
    column = yh * 2 + yl

    def blk_peer(e):
        return (lax.rem(z + e // 8, 4), lax.rem(yh + (e // 4) % 2, 2), lax.rem(x + e % 4, 4), yl, core)

    def plane_peer(e):
        return (lax.rem(z + e // 4, 4), yh, lax.rem(x + e % 4, 4), yl, core)

    def column_peer(d):
        y = lax.rem(column + d, 4)
        return (z, y // 2, x, lax.rem(y, 2), core)

    other_core = (z, yh, x, yl, 1 - core)

    loads = []
    for i in range(8):
        part = pl.ds(i * 1024, 1024)
        loads.append(pltpu.make_async_copy(x_hbm.at[:, part], xin.at[:, part], load_sem))
        loads[-1].start()

    barrier = pltpu.get_barrier_semaphore()
    for e in FAR_FIRST:
        pl.semaphore_signal(barrier, inc=1, device_id=blk_peer(e), device_id_type=MESH)
    for peer in (column_peer(1), column_peer(3), other_core):
        pl.semaphore_signal(barrier, inc=1, device_id=peer, device_id_type=MESH)

    lane, sub = iota(1), iota(0)
    lane_c = lane // 8

    with jax.named_scope("load_wait"):
        pltpu.make_async_copy(x_hbm, xin, load_sem).wait()

    def transpose_some(n, _):
        for k in range(8):
            u = n * 8 + k
            left = xin[:, pl.ds(pl.multiple_of(u * 128 + yh * 4096, 128), 128)]
            right = xin[:, pl.ds(pl.multiple_of(u * 128 + (1 - yh) * 4096, 128), 128)]
            sent[u] = jnp.concatenate([left, right], axis=0).T
        return 0

    with jax.named_scope("transpose"):
        lax.fori_loop(0, 4, transpose_some, 0)
        got[block] = sent[block]
    for tile in range(32):
        sums[tile] = jnp.zeros(VREG, jnp.float32)

    def clear(tile, _):
        for c in range(2):
            for a in range(16):
                acc[tile, c, a] = jnp.zeros(VREG, jnp.float32)
        return 0

    with jax.named_scope("barrier"):
        pl.semaphore_wait(barrier, 34)

    def a_copy(j, e):
        z2, yh2, x2, _, _ = blk_peer(e)
        part = pl.ds(START[j], FIELDS[j] // 2)
        return pltpu.make_async_remote_copy(
            src_ref=sent.at[z2 * 8 + yh2 * 4 + x2, part],
            dst_ref=got.at[block, part],
            send_sem=a_send,
            recv_sem=a_recv.at[j],
            device_id=blk_peer(e),
            device_id_type=MESH,
        )

    def over_peers(act):
        def one(i, _):
            act(lax.rem(i * 13, 32))
            return 0

        lax.fori_loop(1, 32, one, 0)

    with jax.named_scope("send"):
        for e in FAR_FIRST:
            a_copy(0, e).start()
        for j in range(1, ROUNDS):
            over_peers(lambda e: a_copy(j, e).start())

    def tile_at(i, last=True):
        e = sum(jnp.where(i == k, ORDER[k], 0) for k in range(TILES)) if last else i
        return e, lax.rem(z + e // 4, 4) * 4 + lax.rem(x + e % 4, 4)

    def first_block(tile):
        return (tile // 4) * 8 + lax.rem(tile, 4)

    def place():
        here = lax.broadcasted_iota(jnp.int32, (256, 128), 0) % 128
        to = lax.broadcasted_iota(jnp.int32, (256, 128), 1)
        for order in range(5):
            group = (to // 2) % 4 if order == 4 else order
            for side in range(2):
                origin = ((to + side) % 2) * 64 + group * 16 + to // 8
                places[side, :, pl.ds(order * 128, 128)] = jnp.where(here == origin, 1.0, 0.0).astype(jnp.bfloat16)

    def parts(value):
        top = value.astype(jnp.bfloat16)
        return top, (value - top.astype(jnp.float32)).astype(jnp.bfloat16)

    def sides(this, that):
        left = lax.broadcasted_iota(jnp.int32, this.shape, 1) < 64
        return jnp.where(left, this, that), jnp.where(left, that, this)

    def arrange(j):
        half = FIELDS[j] // 2
        pitch = FIELDS[j] + 8
        n = min(32, 1024 // half)

        def split(b, _):
            for k in range(8):
                t = b * 8 + k
                here = pl.ds(pl.multiple_of(t * half, 16), half)
                this = got[t, pl.ds(START[j], half), :]
                for target, value in zip((near, cross), sides(this, got[lax.rem(t + 4, 32), pl.ds(START[j], half), :])):
                    for i, part in enumerate(parts(value)):
                        target[here, pl.ds(i * 128, 128)] = part
                total = sums[t]
                for o in range(half // 8):
                    total = total + this[o * 8 : o * 8 + 8]
                sums[t] = total
            return 0

        def spread_cols(b, _):
            here = pl.ds(pl.multiple_of(b * n * half, 16), n * half)
            for pair in range(2):
                for side, source in enumerate((near, cross)):
                    weight = places[side, :, pl.ds(pair * 256, 256)]
                    value = jnp.dot(source[here, :], weight, preferred_element_type=jnp.float32)
                    for k in range(n):
                        at = ((k // 4 + side) % 2) * half
                        for i in range(2):
                            part = value[k * half : (k + 1) * half, i * 128 : i * 128 + 128]
                            cols[b * n + k, pl.ds((pair * 2 + i) * pitch + at, half), :] = part
            return 0

        def spread_rows(b):
            here = pl.ds(b * 8 * half, 4 * half)
            for side, source in enumerate((near, cross)):
                value = jnp.dot(source[here, :], places[side, :, pl.ds(512, 128)], preferred_element_type=jnp.float32)
                for k in range(4):
                    rows[b * 8 + k, pl.ds(side * half, half), :] = value[k * half : (k + 1) * half]

        lax.fori_loop(0, 4, split, 0)
        lax.fori_loop(0, 32 // n, spread_cols, 0)
        for b in range(4):
            spread_rows(b)

    def turn_field(j, target, r, f):
        row = spread(rows[r, pl.ds(f, 1), :])
        for q in range(2):
            target[f, q] = pltpu.roll(row, 64 * q, 1, stride=8, stride_axis=0)

    def work(j, i, now, later):
        last = j == ROUNDS - 1
        _, tile = tile_at(i, last)
        r = first_block(tile)
        follow = first_block(tile_at(lax.rem(i + 1, TILES), last)[1])
        partner = [lax.rem(r + offset + s, 32) for s in range(4)]
        total = [acc[tile, a // 16, a % 16] for a in range(32)]
        done = 0
        for f in range(FIELDS[j]):
            turned = [now[f, q] for q in range(2)]
            for s in range(4):
                for g in range(4):
                    other = spread(cols[partner[s], pl.ds(g * (FIELDS[j] + 8) + f, 1), :])
                    for q in range(2):
                        a = (g % 2) * 16 + (g // 2) * 8 + s * 2 + q
                        total[a] = total[a] + jnp.minimum(turned[q], other)
            while done < FIELDS[j] and done * (FIELDS[j] - 10) < (f + 1) * FIELDS[j]:
                turn_field(j, later, follow, done)
                done += 1
        for a in range(32):
            acc[tile, a // 16, a % 16] = total[a]

    def first_turn(j):
        r0 = first_block(tile_at(0, j == ROUNDS - 1)[1])

        def some(b, _):
            for f in range(32):
                turn_field(j, roll_a, r0, b * 32 + f)
            return 0

        with jax.named_scope("first"):
            lax.fori_loop(0, FIELDS[j] // 32, some, 0)

    def arrived(j):
        with jax.named_scope("got_wait"):
            part = pl.ds(START[j], FIELDS[j] // 2)
            pltpu.make_async_copy(sent.at[pl.ds(0, 31), part], got.at[pl.ds(0, 31), part], a_recv.at[j]).wait()

    def ready(j):
        arrived(j)
        with jax.named_scope("arrange"):
            arrange(j)
        first_turn(j)

    def round_of(j):
        ready(j)

        def two(i, _):
            work(j, 2 * i, roll_a, roll_b)

            @pl.when(i < TILES)
            def _():
                work(j, 2 * i + 1, roll_b, roll_a)

            return 0

        with jax.named_scope("work"):
            lax.fori_loop(0, TILES // 2, two, 0)

    with jax.named_scope("place"):
        place()
        lax.fori_loop(0, TILES, clear, 0)
    for j in range(ROUNDS - 1):
        round_of(j)
    ready(ROUNDS - 1)

    def total_one(b, _):
        for k in range(8):
            turn[pl.ds(b * 8 + k, 1), :] = jnp.sum(sums[b * 8 + k], axis=0, keepdims=True)
        return 0

    with jax.named_scope("total"):
        lax.fori_loop(0, 4, total_one, 0)
        natural = turn[pl.ds(0, 32), :]
        shifted = jnp.concatenate([natural[4:], natural[:4]], axis=0)
        both = jnp.zeros((32, 128), jnp.float32)
        for side, value in enumerate(sides(natural, shifted)):
            for part in parts(value):
                weight = places[side, pl.ds(0, 128), pl.ds(512, 128)]
                both = both + jnp.dot(part, weight, preferred_element_type=jnp.float32)
        turn[pl.ds(0, 32), :] = both

    def pack_sums(tile, _):
        r = first_block(tile)
        packed = spread(turn[pl.ds(r, 1), :])
        for s in range(4):
            packed = jnp.where(sub == s + 1, spread(turn[pl.ds(lax.rem(r + offset + s, 32), 1), :]), packed)
        for c in range(2):
            acc[tile, c, 16] = packed
        return 0

    with jax.named_scope("pack"):
        lax.fori_loop(0, TILES, pack_sums, 0)

    def core_copy(i):
        _, tile = tile_at(i)
        return pltpu.make_async_remote_copy(
            src_ref=acc.at[tile, 1 - core],
            dst_ref=core_in.at[tile],
            send_sem=c_send,
            recv_sem=c_recv.at[i],
            device_id=other_core,
            device_id_type=MESH,
        )

    def plane_copy(i):
        e, tile = tile_at(i)
        return pltpu.make_async_remote_copy(
            src_ref=acc.at[tile, core],
            dst_ref=plane_in.at[i],
            send_sem=p_send,
            recv_sem=p_recv,
            device_id=plane_peer(e),
            device_id_type=MESH,
        )

    def join_cores(i):
        _, tile = tile_at(i)
        core_copy(i).wait_recv()
        for a in range(17):
            acc[tile, core, a] = acc[tile, core, a] + core_in[tile, a]

    def last_two(i, _):
        work(ROUNDS - 1, 2 * i, roll_a, roll_b)
        core_copy(2 * i).start()
        work(ROUNDS - 1, 2 * i + 1, roll_b, roll_a)
        core_copy(2 * i + 1).start()

        @pl.when(i > 0)
        def _():
            for k in (2 * i - 2, 2 * i - 1):
                join_cores(k)
                plane_copy(k).start()

        return 0

    with jax.named_scope("last_work"):
        lax.fori_loop(0, TILES // 2, last_two, 0)
    with jax.named_scope("last_join"):
        join_cores(TILES - 2)
        plane_copy(TILES - 2).start()
        join_cores(TILES - 1)

    with jax.named_scope("finish"):
        pltpu.make_async_copy(got.at[pl.ds(0, 31)], sent.at[pl.ds(0, 31)], a_send).wait()
    own = z * 4 + x
    whole = [acc[own, core, a] for a in range(17)]
    with jax.named_scope("plane_wait"):
        pltpu.make_async_copy(acc.at[pl.ds(0, 15), 0], plane_in.at[pl.ds(0, 15)], p_recv).wait()
    for i in range(TILES - 1):
        for a in range(17):
            whole[a] = whole[a] + plane_in[i, a]
    for half in range(2):
        for a in range(8):
            column_out[half, a] = whole[half * 8 + a]
        column_out[half, 8] = whole[16]

    def column_copy(d):
        y = lax.rem(column + d, 4)
        return pltpu.make_async_remote_copy(
            src_ref=column_out.at[lax.rem(y, 2)],
            dst_ref=column_in.at[d - 1],
            send_sem=y_send,
            recv_sem=y_recv,
            device_id=column_peer(d),
            device_id_type=MESH,
        )

    for d in (2, 1, 3):
        column_copy(d).start()

    pltpu.make_async_copy(acc.at[:, 0], core_in, c_send).wait()
    pltpu.make_async_copy(acc.at[pl.ds(0, 15), 0], plane_in.at[pl.ds(0, 15)], p_send).wait()
    whole = [column_out[yl, a] for a in range(9)]
    with jax.named_scope("column_wait"):
        pltpu.make_async_copy(column_in, column_in, y_recv).wait()
        pltpu.make_async_copy(column_in, column_in, y_send).wait()
    for d in range(3):
        for a in range(9):
            whole[a] = whole[a] + column_in[d, a]

    with jax.named_scope("end"):
        turn[pl.ds(0, 8), :] = whole[8]
        mine = spread(turn[pl.ds(0, 1), :])
        pick = lane_c * 8 + (yl * 2 + core) * 2 + lane % 2
        theirs = [take(spread(turn[pl.ds(1 + s, 1), :]), pick) for s in range(4)]
        for q in range(2):
            own_sums = pltpu.roll(mine, 64 * q, 1, stride=8, stride_axis=0)
            undo = ((lane_c + sub + 8 * q) % 16) * 8 + lane % 8
            for s in range(4):
                metric = 2.0 * whole[s * 2 + q] / (own_sums + theirs[s])
                flat_out[pl.ds(q * 32 + s, 8, stride=4), :] = take(metric, undo)
        flat = flat_out[pl.ds(0, 64), :]
        turned = jnp.concatenate([flat, flat], axis=0).T
        for i in range(16):
            part = turned[i * 8 : i * 8 + 8, :]
            turn[pl.ds(i * 8, 8), :] = pltpu.roll(part, 4 * i, 1) if i else part
        for i in range(8):
            part = turn[pl.ds((i % 2) * 64 + (i // 2) * 2 + yh, 8, stride=8), :]
            flat_out[pl.ds(i * 8, 8), :] = part
            flat_out[pl.ds(64 + i * 8, 8), :] = part
        turn[...] = flat_out[...].T
        for s in range(4):
            out[pl.ds(s * 16, 16), :] = turn[pl.ds(s, 16, stride=4), :]


def per_device(vectors, section):
    f32 = jnp.float32
    dma = pltpu.SemaphoreType.DMA
    flat = pl.pallas_call(
        kernel,
        out_shape=jax.ShapeDtypeStruct((64, 128), f32),
        in_specs=[pl.BlockSpec(memory_space=pltpu.SMEM), pl.BlockSpec(memory_space=pl.ANY)],
        out_specs=pl.BlockSpec(memory_space=pltpu.VMEM),
        scratch_shapes=[
            pltpu.VMEM((64, 8192), f32),
            pltpu.VMEM((32, 128, 128), f32),
            pltpu.VMEM((32, 128, 128), f32),
            pltpu.VMEM((2, 256, 640), jnp.bfloat16),
            pltpu.VMEM((16 * MOST, 256), jnp.bfloat16),
            pltpu.VMEM((16 * MOST, 256), jnp.bfloat16),
            pltpu.VMEM((32, MOST, 128), f32),
            pltpu.VMEM((32, 4 * (MOST + 8), 128), f32),
            pltpu.VMEM((MOST, 2, 8, 128), f32),
            pltpu.VMEM((MOST, 2, 8, 128), f32),
            pltpu.VMEM((TILES, 2, 17, 8, 128), f32),
            pltpu.VMEM((32, 8, 128), f32),
            pltpu.VMEM((TILES, 17, 8, 128), f32),
            pltpu.VMEM((TILES, 17, 8, 128), f32),
            pltpu.VMEM((2, 9, 8, 128), f32),
            pltpu.VMEM((3, 9, 8, 128), f32),
            pltpu.VMEM((128, 128), f32),
            pltpu.VMEM((128, 128), f32),
            dma,
            dma,
            dma((ROUNDS,)),
            dma,
            dma((TILES,)),
            dma,
            dma,
            dma,
            dma,
        ],
        compiler_params=pltpu.CompilerParams(
            collective_id=0, has_side_effects=True, vmem_limit_bytes=63 * 2**20
        ),
    )(section, vectors)
    return flat[:, :64].reshape(4, 16, 64).transpose(2, 0, 1)


def solution(mesh):
    torus = Mesh(mesh.devices.reshape(4, 2, 4, 2, 2), AXES)
    placed = (P(("z", "yh", "x"), ("yl", "core")), P())
    return jax.shard_map(
        per_device,
        mesh=torus,
        in_specs=placed,
        out_specs=P(("z", "yh", "x"), None, ("yl", "core")),
        check_vma=False,
    )
```

```python
import jax
import jax.numpy as jnp
from jax import lax
from jax.experimental import pallas as pl
from jax.experimental.pallas import tpu as pltpu
from jax.sharding import Mesh
from jax.sharding import PartitionSpec as P

MESH = pl.DeviceIdType.MESH


def hops(e):
    return min(e // 8, 4 - e // 8) + 2 * ((e // 4) % 2) + min(e % 4, 4 - e % 4)


FAR_FIRST = sorted(range(1, 32), key=lambda e: (-hops(e), (e * 13) % 32))
AXES = ("z", "yh", "x", "yl", "core")
FIELDS = (32, 64, 32, 128)
ROUNDS = len(FIELDS)
START = [sum(FIELDS[:j]) // 2 for j in range(ROUNDS)]
MOST = max(FIELDS)
TILES = 16
ORDER = (10, 9, 11, 6, 14, 5, 7, 13, 15, 2, 8, 1, 12, 3, 4, 0)
VREG = (8, 128)


def iota(axis):
    return lax.broadcasted_iota(jnp.int32, VREG, axis)


def spread(row):
    return jnp.broadcast_to(row, VREG)


def take(value, index):
    return jnp.take_along_axis(value, index, axis=1)


def kernel(
    section, x_hbm, out, xin, sent, got, places, near, cross, rows, cols, roll_a, roll_b, acc, sums, core_in, plane_in, column_out, column_in,
    turn, flat_out, load_sem, a_send, a_recv, c_send, c_recv, p_send, p_recv, y_send, y_recv,
):
    z, yh, x, yl, core = (lax.axis_index(name) for name in AXES)
    offset = section[0]
    block = z * 8 + yh * 4 + x
    column = yh * 2 + yl

    def blk_peer(e):
        return (lax.rem(z + lax.div(e, 8), 4), lax.rem(yh + lax.div(e, 4), 2), lax.rem(x + e, 4), yl, core)

    def plane_peer(e):
        return (lax.rem(z + lax.div(e, 4), 4), yh, lax.rem(x + e, 4), yl, core)

    def column_peer(d):
        y = lax.rem(column + d, 4)
        return (z, lax.div(y, 2), x, lax.rem(y, 2), core)

    other_core = (z, yh, x, yl, 1 - core)

    loads = []
    for i in range(8):
        part = pl.ds(i * 1024, 1024)
        loads.append(pltpu.make_async_copy(x_hbm.at[:, part], xin.at[:, part], load_sem))
        loads[-1].start()

    barrier = pltpu.get_barrier_semaphore()
    for e in FAR_FIRST:
        pl.semaphore_signal(barrier, inc=1, device_id=blk_peer(e), device_id_type=MESH)
    for peer in (column_peer(1), column_peer(3), other_core):
        pl.semaphore_signal(barrier, inc=1, device_id=peer, device_id_type=MESH)

    lane, sub = iota(1), iota(0)
    lane_c = lane // 8

    with jax.named_scope("load_wait"):
        pltpu.make_async_copy(x_hbm, xin, load_sem).wait()

    def transpose_some(n, _):
        for k in range(8):
            u = n * 8 + k
            left = xin[:, pl.ds(pl.multiple_of(u * 128 + yh * 4096, 128), 128)]
            right = xin[:, pl.ds(pl.multiple_of(u * 128 + (1 - yh) * 4096, 128), 128)]
            sent[u] = jnp.concatenate([left, right], axis=0).T
        return 0

    with jax.named_scope("transpose"):
        lax.fori_loop(0, 4, transpose_some, 0)
        got[block] = sent[block]
    for tile in range(32):
        sums[tile] = jnp.zeros(VREG, jnp.float32)

    def clear(tile, _):
        for c in range(2):
            for a in range(16):
                acc[tile, c, a] = jnp.zeros(VREG, jnp.float32)
        return 0

    with jax.named_scope("barrier"):
        pl.semaphore_wait(barrier, 34)

    def a_copy(j, e):
        z2, yh2, x2, _, _ = blk_peer(e)
        part = pl.ds(START[j], FIELDS[j] // 2)
        return pltpu.make_async_remote_copy(
            src_ref=sent.at[z2 * 8 + yh2 * 4 + x2, part],
            dst_ref=got.at[block, part],
            send_sem=a_send,
            recv_sem=a_recv.at[j],
            device_id=blk_peer(e),
            device_id_type=MESH,
        )

    def over_peers(act):
        def one(i, _):
            act(lax.rem(i * 13, 32))
            return 0

        lax.fori_loop(1, 32, one, 0)

    with jax.named_scope("send"):
        for e in FAR_FIRST:
            a_copy(0, e).start()
        for j in range(1, ROUNDS):
            over_peers(lambda e: a_copy(j, e).start())

    def tile_at(i):
        e = sum(jnp.where(i == k, ORDER[k], 0) for k in range(TILES))
        return e, lax.rem(z + lax.div(e, 4), 4) * 4 + lax.rem(x + e, 4)

    def first_block(tile):
        return 2 * tile - lax.rem(tile, 4)

    def place():
        here = lax.broadcasted_iota(jnp.int32, (256, 128), 0) % 128
        to = lax.broadcasted_iota(jnp.int32, (256, 128), 1)
        for order in range(5):
            group = (to // 2) % 4 if order == 4 else order
            for side in range(2):
                origin = ((to + side) % 2) * 64 + group * 16 + to // 8
                places[side, :, pl.ds(order * 128, 128)] = jnp.where(here == origin, 1.0, 0.0).astype(jnp.bfloat16)

    def parts(value):
        top = value.astype(jnp.bfloat16)
        return top, (value - top.astype(jnp.float32)).astype(jnp.bfloat16)

    def sides(this, that):
        left = lax.broadcasted_iota(jnp.int32, this.shape, 1) < 64
        return jnp.where(left, this, that), jnp.where(left, that, this)

    def arrange(j):
        half = FIELDS[j] // 2
        pitch = FIELDS[j] + 8
        n = min(32, 1024 // half)

        def split(b, _):
            for k in range(8):
                t = b * 8 + k
                here = pl.ds(pl.multiple_of(t * half, 16), half)
                this = got[t, pl.ds(START[j], half), :]
                for target, value in zip((near, cross), sides(this, got[lax.rem(t + 4, 32), pl.ds(START[j], half), :])):
                    for i, part in enumerate(parts(value)):
                        target[here, pl.ds(i * 128, 128)] = part
                total = sums[t]
                for o in range(half // 8):
                    total = total + this[o * 8 : o * 8 + 8]
                sums[t] = total
            return 0

        def spread_cols(b, _):
            here = pl.ds(pl.multiple_of(b * n * half, 16), n * half)
            for pair in range(2):
                for side, source in enumerate((near, cross)):
                    weight = places[side, :, pl.ds(pair * 256, 256)]
                    value = jnp.dot(source[here, :], weight, preferred_element_type=jnp.float32)
                    for k in range(n):
                        at = ((k // 4 + side) % 2) * half
                        for i in range(2):
                            part = value[k * half : (k + 1) * half, i * 128 : i * 128 + 128]
                            cols[b * n + k, pl.ds((pair * 2 + i) * pitch + at, half), :] = part
            return 0

        def spread_rows(b):
            here = pl.ds(b * 8 * half, 4 * half)
            for side, source in enumerate((near, cross)):
                value = jnp.dot(source[here, :], places[side, :, pl.ds(512, 128)], preferred_element_type=jnp.float32)
                for k in range(4):
                    rows[b * 8 + k, pl.ds(side * half, half), :] = value[k * half : (k + 1) * half]

        lax.fori_loop(0, 4, split, 0)
        lax.fori_loop(0, 32 // n, spread_cols, 0)
        for b in range(4):
            spread_rows(b)

    def turn_field(j, target, r, f):
        row = spread(rows[r, pl.ds(f, 1), :])
        for q in range(2):
            target[f, q] = pltpu.roll(row, 64 * q, 1, stride=8, stride_axis=0)

    def work(j, i, now, later):
        after = lax.rem(i + 1, TILES)
        if j == ROUNDS - 1:
            tile, after = tile_at(i)[1], tile_at(after)[1]
        else:
            tile = i
        r, follow = first_block(tile), first_block(after)
        partner = [lax.rem(r + offset + s, 32) for s in range(4)]
        total = [acc[tile, a // 16, a % 16] for a in range(32)]
        done = 0
        for f in range(FIELDS[j]):
            turned = [now[f, q] for q in range(2)]
            for s in range(4):
                for g in range(4):
                    other = spread(cols[partner[s], pl.ds(g * (FIELDS[j] + 8) + f, 1), :])
                    for q in range(2):
                        a = (g % 2) * 16 + (g // 2) * 8 + s * 2 + q
                        total[a] = total[a] + jnp.minimum(turned[q], other)
            while done < FIELDS[j] and done * (FIELDS[j] - 10) < (f + 1) * FIELDS[j]:
                turn_field(j, later, follow, done)
                done += 1
        for a in range(32):
            acc[tile, a // 16, a % 16] = total[a]

    def first_turn(j):
        r0 = first_block(tile_at(0)[1] if j == ROUNDS - 1 else 0)

        def some(b, _):
            for f in range(32):
                turn_field(j, roll_a, r0, b * 32 + f)
            return 0

        with jax.named_scope("first"):
            lax.fori_loop(0, FIELDS[j] // 32, some, 0)

    def arrived(j):
        with jax.named_scope("got_wait"):
            part = pl.ds(START[j], FIELDS[j] // 2)
            pltpu.make_async_copy(sent.at[pl.ds(0, 31), part], got.at[pl.ds(0, 31), part], a_recv.at[j]).wait()

    def ready(j):
        arrived(j)
        with jax.named_scope("arrange"):
            arrange(j)
        first_turn(j)

    def round_of(j):
        ready(j)

        def two(i, _):
            work(j, 2 * i, roll_a, roll_b)

            @pl.when(i < TILES)
            def _():
                work(j, 2 * i + 1, roll_b, roll_a)

            return 0

        with jax.named_scope("work"):
            lax.fori_loop(0, TILES // 2, two, 0)

    with jax.named_scope("place"):
        place()
        lax.fori_loop(0, TILES, clear, 0)
    for j in range(ROUNDS - 1):
        round_of(j)
    ready(ROUNDS - 1)

    def total_one(b, _):
        for k in range(8):
            turn[pl.ds(b * 8 + k, 1), :] = jnp.sum(sums[b * 8 + k], axis=0, keepdims=True)
        return 0

    with jax.named_scope("total"):
        lax.fori_loop(0, 4, total_one, 0)
        natural = turn[pl.ds(0, 32), :]
        shifted = jnp.concatenate([natural[4:], natural[:4]], axis=0)
        both = jnp.zeros((32, 128), jnp.float32)
        for side, value in enumerate(sides(natural, shifted)):
            for part in parts(value):
                weight = places[side, pl.ds(0, 128), pl.ds(512, 128)]
                both = both + jnp.dot(part, weight, preferred_element_type=jnp.float32)
        turn[pl.ds(0, 32), :] = both

    def pack_sums(tile, _):
        r = first_block(tile)
        packed = spread(turn[pl.ds(r, 1), :])
        for s in range(4):
            packed = jnp.where(sub == s + 1, spread(turn[pl.ds(lax.rem(r + offset + s, 32), 1), :]), packed)
        for c in range(2):
            acc[tile, c, 16] = packed
        return 0

    with jax.named_scope("pack"):
        lax.fori_loop(0, TILES, pack_sums, 0)

    def core_copy(i):
        _, tile = tile_at(i)
        return pltpu.make_async_remote_copy(
            src_ref=acc.at[tile, 1 - core],
            dst_ref=core_in.at[tile],
            send_sem=c_send,
            recv_sem=c_recv.at[i],
            device_id=other_core,
            device_id_type=MESH,
        )

    def plane_copy(i):
        e, tile = tile_at(i)
        return pltpu.make_async_remote_copy(
            src_ref=acc.at[tile, core],
            dst_ref=plane_in.at[i],
            send_sem=p_send,
            recv_sem=p_recv,
            device_id=plane_peer(e),
            device_id_type=MESH,
        )

    def join_cores(i):
        _, tile = tile_at(i)
        core_copy(i).wait_recv()
        for a in range(17):
            acc[tile, core, a] = acc[tile, core, a] + core_in[tile, a]

    def last_two(i, _):
        work(ROUNDS - 1, 2 * i, roll_a, roll_b)
        core_copy(2 * i).start()
        work(ROUNDS - 1, 2 * i + 1, roll_b, roll_a)
        core_copy(2 * i + 1).start()

        @pl.when(i > 0)
        def _():
            for k in (2 * i - 2, 2 * i - 1):
                join_cores(k)
                plane_copy(k).start()

        return 0

    with jax.named_scope("last_work"):
        lax.fori_loop(0, TILES // 2, last_two, 0)
    with jax.named_scope("last_join"):
        join_cores(TILES - 2)
        plane_copy(TILES - 2).start()
        join_cores(TILES - 1)

    with jax.named_scope("finish"):
        pltpu.make_async_copy(got.at[pl.ds(0, 31)], sent.at[pl.ds(0, 31)], a_send).wait()
    own = z * 4 + x
    whole = [acc[own, core, a] for a in range(17)]
    with jax.named_scope("plane_wait"):
        pltpu.make_async_copy(acc.at[pl.ds(0, 15), 0], plane_in.at[pl.ds(0, 15)], p_recv).wait()
    for i in range(TILES - 1):
        for a in range(17):
            whole[a] = whole[a] + plane_in[i, a]
    for half in range(2):
        for a in range(8):
            column_out[half, a] = whole[half * 8 + a]
        column_out[half, 8] = whole[16]

    def column_copy(d):
        y = lax.rem(column + d, 4)
        return pltpu.make_async_remote_copy(
            src_ref=column_out.at[lax.rem(y, 2)],
            dst_ref=column_in.at[d - 1],
            send_sem=y_send,
            recv_sem=y_recv,
            device_id=column_peer(d),
            device_id_type=MESH,
        )

    for d in (2, 1, 3):
        column_copy(d).start()

    pltpu.make_async_copy(acc.at[:, 0], core_in, c_send).wait()
    pltpu.make_async_copy(acc.at[pl.ds(0, 15), 0], plane_in.at[pl.ds(0, 15)], p_send).wait()
    whole = [column_out[yl, a] for a in range(9)]
    with jax.named_scope("column_wait"):
        pltpu.make_async_copy(column_in, column_in, y_recv).wait()
        pltpu.make_async_copy(column_in, column_in, y_send).wait()
    for d in range(3):
        for a in range(9):
            whole[a] = whole[a] + column_in[d, a]

    with jax.named_scope("end"):
        turn[pl.ds(0, 8), :] = whole[8]
        mine = spread(turn[pl.ds(0, 1), :])
        pick = lane_c * 8 + (yl * 2 + core) * 2 + lane % 2
        theirs = [take(spread(turn[pl.ds(1 + s, 1), :]), pick) for s in range(4)]
        for q in range(2):
            own_sums = pltpu.roll(mine, 64 * q, 1, stride=8, stride_axis=0)
            undo = ((lane_c + sub + 8 * q) % 16) * 8 + lane % 8
            for s in range(4):
                metric = 2.0 * whole[s * 2 + q] / (own_sums + theirs[s])
                flat_out[pl.ds(q * 32 + s, 8, stride=4), :] = take(metric, undo)
        flat = flat_out[pl.ds(0, 64), :]
        turned = jnp.concatenate([flat, flat], axis=0).T
        for i in range(16):
            part = turned[i * 8 : i * 8 + 8, :]
            turn[pl.ds(i * 8, 8), :] = pltpu.roll(part, 4 * i, 1) if i else part
        for i in range(8):
            part = turn[pl.ds((i % 2) * 64 + (i // 2) * 2 + yh, 8, stride=8), :]
            flat_out[pl.ds(i * 8, 8), :] = part
            flat_out[pl.ds(64 + i * 8, 8), :] = part
        turn[...] = flat_out[...].T
        for s in range(4):
            out[pl.ds(s * 16, 16), :] = turn[pl.ds(s, 16, stride=4), :]


def per_device(vectors, section):
    f32 = jnp.float32
    dma = pltpu.SemaphoreType.DMA
    flat = pl.pallas_call(
        kernel,
        out_shape=jax.ShapeDtypeStruct((64, 128), f32),
        in_specs=[pl.BlockSpec(memory_space=pltpu.SMEM), pl.BlockSpec(memory_space=pl.ANY)],
        out_specs=pl.BlockSpec(memory_space=pltpu.VMEM),
        scratch_shapes=[
            pltpu.VMEM((64, 8192), f32),
            pltpu.VMEM((32, 128, 128), f32),
            pltpu.VMEM((32, 128, 128), f32),
            pltpu.VMEM((2, 256, 640), jnp.bfloat16),
            pltpu.VMEM((16 * MOST, 256), jnp.bfloat16),
            pltpu.VMEM((16 * MOST, 256), jnp.bfloat16),
            pltpu.VMEM((32, MOST, 128), f32),
            pltpu.VMEM((32, 4 * (MOST + 8), 128), f32),
            pltpu.VMEM((MOST, 2, 8, 128), f32),
            pltpu.VMEM((MOST, 2, 8, 128), f32),
            pltpu.VMEM((TILES, 2, 17, 8, 128), f32),
            pltpu.VMEM((32, 8, 128), f32),
            pltpu.VMEM((TILES, 17, 8, 128), f32),
            pltpu.VMEM((TILES, 17, 8, 128), f32),
            pltpu.VMEM((2, 9, 8, 128), f32),
            pltpu.VMEM((3, 9, 8, 128), f32),
            pltpu.VMEM((128, 128), f32),
            pltpu.VMEM((128, 128), f32),
            dma,
            dma,
            dma((ROUNDS,)),
            dma,
            dma((TILES,)),
            dma,
            dma,
            dma,
            dma,
        ],
        compiler_params=pltpu.CompilerParams(
            collective_id=0, has_side_effects=True, vmem_limit_bytes=63 * 2**20
        ),
    )(section, vectors)
    return flat[:, :64].reshape(4, 16, 64).transpose(2, 0, 1)


def solution(mesh):
    torus = Mesh(mesh.devices.reshape(4, 2, 4, 2, 2), AXES)
    placed = (P(("z", "yh", "x"), ("yl", "core")), P())
    return jax.shard_map(
        per_device,
        mesh=torus,
        in_specs=placed,
        out_specs=P(("z", "yh", "x"), None, ("yl", "core")),
        check_vma=False,
    )
```

```python
import jax
import jax.numpy as jnp
from jax import lax
from jax.experimental import pallas as pl
from jax.experimental.pallas import tpu as pltpu
from jax.sharding import Mesh
from jax.sharding import PartitionSpec as P

MESH = pl.DeviceIdType.MESH


def hops(e):
    return min(e // 8, 4 - e // 8) + 2 * ((e // 4) % 2) + min(e % 4, 4 - e % 4)


FAR_FIRST = sorted(range(1, 32), key=lambda e: (-hops(e), (e * 13) % 32))
AXES = ("z", "yh", "x", "yl", "core")
FIELDS = (32, 32, 64, 128)
ROUNDS = len(FIELDS)
START = [sum(FIELDS[:j]) // 2 for j in range(ROUNDS)]
MOST = max(FIELDS)
TILES = 16
ORDER = (10, 9, 11, 6, 14, 5, 7, 13, 15, 2, 8, 1, 12, 3, 4, 0)
VREG = (8, 128)


def iota(axis):
    return lax.broadcasted_iota(jnp.int32, VREG, axis)


def spread(row):
    return jnp.broadcast_to(row, VREG)


def take(value, index):
    return jnp.take_along_axis(value, index, axis=1)


def kernel(
    section, x_hbm, out, xin, sent, got, places, near, cross, rows, cols, roll_a, roll_b, acc, sums, core_in, plane_in, column_out, column_in,
    turn, flat_out, load_sem, a_send, a_recv, c_send, c_recv, p_send, p_recv, y_send, y_recv,
):
    z, yh, x, yl, core = (lax.axis_index(name) for name in AXES)
    offset = section[0]
    block = z * 8 + yh * 4 + x
    column = yh * 2 + yl

    def blk_peer(e):
        return (lax.rem(z + lax.div(e, 8), 4), lax.rem(yh + lax.div(e, 4), 2), lax.rem(x + e, 4), yl, core)

    def plane_peer(e):
        return (lax.rem(z + lax.div(e, 4), 4), yh, lax.rem(x + e, 4), yl, core)

    def column_peer(d):
        y = lax.rem(column + d, 4)
        return (z, lax.div(y, 2), x, lax.rem(y, 2), core)

    other_core = (z, yh, x, yl, 1 - core)

    loads = []
    for i in range(8):
        part = pl.ds(i * 1024, 1024)
        loads.append(pltpu.make_async_copy(x_hbm.at[:, part], xin.at[:, part], load_sem))
        loads[-1].start()

    barrier = pltpu.get_barrier_semaphore()
    for e in FAR_FIRST:
        pl.semaphore_signal(barrier, inc=1, device_id=blk_peer(e), device_id_type=MESH)
    for peer in (column_peer(1), column_peer(3), other_core):
        pl.semaphore_signal(barrier, inc=1, device_id=peer, device_id_type=MESH)

    lane, sub = iota(1), iota(0)
    lane_c = lane // 8

    with jax.named_scope("load_wait"):
        pltpu.make_async_copy(x_hbm, xin, load_sem).wait()

    def transpose_some(n, _):
        for k in range(8):
            u = n * 8 + k
            left = xin[:, pl.ds(pl.multiple_of(u * 128 + yh * 4096, 128), 128)]
            right = xin[:, pl.ds(pl.multiple_of(u * 128 + (1 - yh) * 4096, 128), 128)]
            sent[u] = jnp.concatenate([left, right], axis=0).T
        return 0

    with jax.named_scope("transpose"):
        lax.fori_loop(0, 4, transpose_some, 0)
        got[block] = sent[block]
    for tile in range(32):
        sums[tile] = jnp.zeros(VREG, jnp.float32)

    def clear(tile, _):
        for c in range(2):
            for a in range(16):
                acc[tile, c, a] = jnp.zeros(VREG, jnp.float32)
        return 0

    with jax.named_scope("barrier"):
        pl.semaphore_wait(barrier, 34)

    def a_copy(j, e):
        z2, yh2, x2, _, _ = blk_peer(e)
        part = pl.ds(START[j], FIELDS[j] // 2)
        return pltpu.make_async_remote_copy(
            src_ref=sent.at[z2 * 8 + yh2 * 4 + x2, part],
            dst_ref=got.at[block, part],
            send_sem=a_send,
            recv_sem=a_recv.at[j],
            device_id=blk_peer(e),
            device_id_type=MESH,
        )

    def over_peers(act):
        def one(i, _):
            act(lax.rem(i * 13, 32))
            return 0

        lax.fori_loop(1, 32, one, 0)

    with jax.named_scope("send"):
        for e in FAR_FIRST:
            a_copy(0, e).start()
        for j in range(1, ROUNDS):
            over_peers(lambda e: a_copy(j, e).start())

    def tile_at(i):
        e = sum(jnp.where(i == k, ORDER[k], 0) for k in range(TILES))
        return e, lax.rem(z + lax.div(e, 4), 4) * 4 + lax.rem(x + e, 4)

    def first_block(tile):
        return 2 * tile - lax.rem(tile, 4)

    def place():
        here = lax.broadcasted_iota(jnp.int32, (256, 128), 0) % 128
        to = lax.broadcasted_iota(jnp.int32, (256, 128), 1)
        for order in range(5):
            group = (to // 2) % 4 if order == 4 else order
            for side in range(2):
                origin = ((to + side) % 2) * 64 + group * 16 + to // 8
                places[side, :, pl.ds(order * 128, 128)] = jnp.where(here == origin, 1.0, 0.0).astype(jnp.bfloat16)

    def parts(value):
        top = value.astype(jnp.bfloat16)
        return top, (value - top.astype(jnp.float32)).astype(jnp.bfloat16)

    def sides(this, that):
        left = lax.broadcasted_iota(jnp.int32, this.shape, 1) < 64
        return jnp.where(left, this, that), jnp.where(left, that, this)

    def arrange(j):
        half = FIELDS[j] // 2
        pitch = FIELDS[j] + 8
        n = min(32, 1024 // half)
        some = 4 if half > 32 else 8

        def split(b, _):
            for k in range(some):
                t = b * some + k
                here = pl.ds(pl.multiple_of(t * half, 16), half)
                this = got[t, pl.ds(START[j], half), :]
                for target, value in zip((near, cross), sides(this, got[lax.rem(t + 4, 32), pl.ds(START[j], half), :])):
                    for i, part in enumerate(parts(value)):
                        target[here, pl.ds(i * 128, 128)] = part
                total = sums[t]
                for o in range(half // 8):
                    total = total + this[o * 8 : o * 8 + 8]
                sums[t] = total
            return 0

        def spread_cols(b, _):
            here = pl.ds(pl.multiple_of(b * n * half, 16), n * half)
            for pair in range(2):
                for side, source in enumerate((near, cross)):
                    weight = places[side, :, pl.ds(pair * 256, 256)]
                    value = jnp.dot(source[here, :], weight, preferred_element_type=jnp.float32)
                    for k in range(n):
                        at = ((k // 4 + side) % 2) * half
                        for i in range(2):
                            part = value[k * half : (k + 1) * half, i * 128 : i * 128 + 128]
                            cols[b * n + k, pl.ds((pair * 2 + i) * pitch + at, half), :] = part
            return 0

        def spread_rows(b):
            here = pl.ds(b * 8 * half, 4 * half)
            for side, source in enumerate((near, cross)):
                value = jnp.dot(source[here, :], places[side, :, pl.ds(512, 128)], preferred_element_type=jnp.float32)
                for k in range(4):
                    rows[b * 8 + k, pl.ds(side * half, half), :] = value[k * half : (k + 1) * half]

        lax.fori_loop(0, 32 // some, split, 0)
        lax.fori_loop(0, 32 // n, spread_cols, 0)
        for b in range(4):
            spread_rows(b)

    def turn_field(j, target, r, f):
        row = spread(rows[r, pl.ds(f, 1), :])
        for q in range(2):
            target[f, q] = pltpu.roll(row, 64 * q, 1, stride=8, stride_axis=0)

    def work(j, i, now, later):
        after = lax.rem(i + 1, TILES)
        if j == ROUNDS - 1:
            tile, after = tile_at(i)[1], tile_at(after)[1]
        else:
            tile = i
        r, follow = first_block(tile), first_block(after)
        partner = [lax.rem(r + offset + s, 32) for s in range(4)]
        total = [acc[tile, a // 16, a % 16] for a in range(32)]
        done = 0
        for f in range(FIELDS[j]):
            turned = [now[f, q] for q in range(2)]
            for s in range(4):
                for g in range(4):
                    other = spread(cols[partner[s], pl.ds(g * (FIELDS[j] + 8) + f, 1), :])
                    for q in range(2):
                        a = (g % 2) * 16 + (g // 2) * 8 + s * 2 + q
                        total[a] = total[a] + jnp.minimum(turned[q], other)
            while done < FIELDS[j] and done * (FIELDS[j] - 10) < (f + 1) * FIELDS[j]:
                turn_field(j, later, follow, done)
                done += 1
        for a in range(32):
            acc[tile, a // 16, a % 16] = total[a]

    def first_turn(j):
        r0 = first_block(tile_at(0)[1] if j == ROUNDS - 1 else 0)

        def some(b, _):
            for f in range(min(FIELDS[j], 64)):
                turn_field(j, roll_a, r0, b * 64 + f)
            return 0

        with jax.named_scope("first"):
            lax.fori_loop(0, max(FIELDS[j] // 64, 1), some, 0)

    def arrived(j):
        with jax.named_scope("got_wait"):
            part = pl.ds(START[j], FIELDS[j] // 2)
            pltpu.make_async_copy(sent.at[pl.ds(0, 31), part], got.at[pl.ds(0, 31), part], a_recv.at[j]).wait()

    def ready(j):
        arrived(j)
        with jax.named_scope("arrange"):
            arrange(j)
        first_turn(j)

    def round_of(j):
        ready(j)

        def two(i, _):
            work(j, 2 * i, roll_a, roll_b)

            @pl.when(i < TILES)
            def _():
                work(j, 2 * i + 1, roll_b, roll_a)

            return 0

        with jax.named_scope("work"):
            lax.fori_loop(0, TILES // 2, two, 0)

    with jax.named_scope("place"):
        place()
        lax.fori_loop(0, TILES, clear, 0)
    for j in range(ROUNDS - 1):
        round_of(j)
    ready(ROUNDS - 1)

    def total_one(b, _):
        for k in range(8):
            turn[pl.ds(b * 8 + k, 1), :] = jnp.sum(sums[b * 8 + k], axis=0, keepdims=True)
        return 0

    with jax.named_scope("total"):
        lax.fori_loop(0, 4, total_one, 0)
        natural = turn[pl.ds(0, 32), :]
        shifted = jnp.concatenate([natural[4:], natural[:4]], axis=0)
        both = jnp.zeros((32, 128), jnp.float32)
        for side, value in enumerate(sides(natural, shifted)):
            for part in parts(value):
                weight = places[side, pl.ds(0, 128), pl.ds(512, 128)]
                both = both + jnp.dot(part, weight, preferred_element_type=jnp.float32)
        turn[pl.ds(0, 32), :] = both

    def pack_sums(tile, _):
        r = first_block(tile)
        packed = spread(turn[pl.ds(r, 1), :])
        for s in range(4):
            packed = jnp.where(sub == s + 1, spread(turn[pl.ds(lax.rem(r + offset + s, 32), 1), :]), packed)
        for c in range(2):
            acc[tile, c, 16] = packed
        return 0

    with jax.named_scope("pack"):
        lax.fori_loop(0, TILES, pack_sums, 0)

    def core_copy(i):
        _, tile = tile_at(i)
        return pltpu.make_async_remote_copy(
            src_ref=acc.at[tile, 1 - core],
            dst_ref=core_in.at[tile],
            send_sem=c_send,
            recv_sem=c_recv.at[i],
            device_id=other_core,
            device_id_type=MESH,
        )

    def plane_copy(i):
        e, tile = tile_at(i)
        return pltpu.make_async_remote_copy(
            src_ref=acc.at[tile, core],
            dst_ref=plane_in.at[i],
            send_sem=p_send,
            recv_sem=p_recv,
            device_id=plane_peer(e),
            device_id_type=MESH,
        )

    def join_cores(i):
        _, tile = tile_at(i)
        core_copy(i).wait_recv()
        for a in range(17):
            acc[tile, core, a] = acc[tile, core, a] + core_in[tile, a]

    def last_two(i, _):
        work(ROUNDS - 1, 2 * i, roll_a, roll_b)
        core_copy(2 * i).start()
        work(ROUNDS - 1, 2 * i + 1, roll_b, roll_a)
        core_copy(2 * i + 1).start()

        @pl.when(i > 0)
        def _():
            for k in (2 * i - 2, 2 * i - 1):
                join_cores(k)
                plane_copy(k).start()

        return 0

    with jax.named_scope("last_work"):
        lax.fori_loop(0, TILES // 2, last_two, 0)
    with jax.named_scope("last_join"):
        join_cores(TILES - 2)
        plane_copy(TILES - 2).start()
        join_cores(TILES - 1)

    with jax.named_scope("finish"):
        pltpu.make_async_copy(got.at[pl.ds(0, 31)], sent.at[pl.ds(0, 31)], a_send).wait()
    own = z * 4 + x
    whole = [acc[own, core, a] for a in range(17)]
    with jax.named_scope("plane_wait"):
        pltpu.make_async_copy(acc.at[pl.ds(0, 15), 0], plane_in.at[pl.ds(0, 15)], p_recv).wait()
    for i in range(TILES - 1):
        for a in range(17):
            whole[a] = whole[a] + plane_in[i, a]
    for half in range(2):
        for a in range(8):
            column_out[half, a] = whole[half * 8 + a]
        column_out[half, 8] = whole[16]

    def column_copy(d):
        y = lax.rem(column + d, 4)
        return pltpu.make_async_remote_copy(
            src_ref=column_out.at[lax.rem(y, 2)],
            dst_ref=column_in.at[d - 1],
            send_sem=y_send,
            recv_sem=y_recv,
            device_id=column_peer(d),
            device_id_type=MESH,
        )

    for d in (2, 1, 3):
        column_copy(d).start()

    pltpu.make_async_copy(acc.at[:, 0], core_in, c_send).wait()
    pltpu.make_async_copy(acc.at[pl.ds(0, 15), 0], plane_in.at[pl.ds(0, 15)], p_send).wait()
    whole = [column_out[yl, a] for a in range(9)]
    with jax.named_scope("column_wait"):
        pltpu.make_async_copy(column_in, column_in, y_recv).wait()
        pltpu.make_async_copy(column_in, column_in, y_send).wait()
    for d in range(3):
        for a in range(9):
            whole[a] = whole[a] + column_in[d, a]

    with jax.named_scope("end"):
        turn[pl.ds(0, 8), :] = whole[8]
        mine = spread(turn[pl.ds(0, 1), :])
        pick = lane_c * 8 + (yl * 2 + core) * 2 + lane % 2
        theirs = [take(spread(turn[pl.ds(1 + s, 1), :]), pick) for s in range(4)]
        for q in range(2):
            own_sums = pltpu.roll(mine, 64 * q, 1, stride=8, stride_axis=0)
            undo = ((lane_c + sub + 8 * q) % 16) * 8 + lane % 8
            for s in range(4):
                metric = 2.0 * whole[s * 2 + q] / (own_sums + theirs[s])
                flat_out[pl.ds(q * 32 + s, 8, stride=4), :] = take(metric, undo)
        flat = flat_out[pl.ds(0, 64), :]
        turned = jnp.concatenate([flat, flat], axis=0).T
        for i in range(16):
            part = turned[i * 8 : i * 8 + 8, :]
            turn[pl.ds(i * 8, 8), :] = pltpu.roll(part, 4 * i, 1) if i else part
        for i in range(8):
            part = turn[pl.ds((i % 2) * 64 + (i // 2) * 2 + yh, 8, stride=8), :]
            flat_out[pl.ds(i * 8, 8), :] = part
            flat_out[pl.ds(64 + i * 8, 8), :] = part
        turn[...] = flat_out[...].T
        for s in range(4):
            out[pl.ds(s * 16, 16), :] = turn[pl.ds(s, 16, stride=4), :]


def per_device(vectors, section):
    f32 = jnp.float32
    dma = pltpu.SemaphoreType.DMA
    flat = pl.pallas_call(
        kernel,
        out_shape=jax.ShapeDtypeStruct((64, 128), f32),
        in_specs=[pl.BlockSpec(memory_space=pltpu.SMEM), pl.BlockSpec(memory_space=pl.ANY)],
        out_specs=pl.BlockSpec(memory_space=pltpu.VMEM),
        scratch_shapes=[
            pltpu.VMEM((64, 8192), f32),
            pltpu.VMEM((32, 128, 128), f32),
            pltpu.VMEM((32, 128, 128), f32),
            pltpu.VMEM((2, 256, 640), jnp.bfloat16),
            pltpu.VMEM((16 * MOST, 256), jnp.bfloat16),
            pltpu.VMEM((16 * MOST, 256), jnp.bfloat16),
            pltpu.VMEM((32, MOST, 128), f32),
            pltpu.VMEM((32, 4 * (MOST + 8), 128), f32),
            pltpu.VMEM((MOST, 2, 8, 128), f32),
            pltpu.VMEM((MOST, 2, 8, 128), f32),
            pltpu.VMEM((TILES, 2, 17, 8, 128), f32),
            pltpu.VMEM((32, 8, 128), f32),
            pltpu.VMEM((TILES, 17, 8, 128), f32),
            pltpu.VMEM((TILES, 17, 8, 128), f32),
            pltpu.VMEM((2, 9, 8, 128), f32),
            pltpu.VMEM((3, 9, 8, 128), f32),
            pltpu.VMEM((128, 128), f32),
            pltpu.VMEM((128, 128), f32),
            dma,
            dma,
            dma((ROUNDS,)),
            dma,
            dma((TILES,)),
            dma,
            dma,
            dma,
            dma,
        ],
        compiler_params=pltpu.CompilerParams(
            collective_id=0, has_side_effects=True, vmem_limit_bytes=63 * 2**20
        ),
    )(section, vectors)
    return flat[:, :64].reshape(4, 16, 64).transpose(2, 0, 1)


def solution(mesh):
    torus = Mesh(mesh.devices.reshape(4, 2, 4, 2, 2), AXES)
    placed = (P(("z", "yh", "x"), ("yl", "core")), P())
    return jax.shard_map(
        per_device,
        mesh=torus,
        in_specs=placed,
        out_specs=P(("z", "yh", "x"), None, ("yl", "core")),
        check_vma=False,
    )
```
